32 devices in a mesh: data: 2 (over x), col: 4 (over z), row: 4 (over y, core).
Axes of the slice: x: 2, y: 2, z: 4, core: 2. Of those that a mesh axis runs over, the one named last changes fastest.
Arguments:
- x: bfloat16 [16, 64, 4096], P(None, 'data', 'row'), parts along dimension 1
- w_x1: bfloat16 [2, 4096, 16384], P(None, 'row', 'col')
- w_h1: bfloat16 [2, 4096, 16384], P(None, 'row', 'col')
- b_1: float32 [2, 16384], P(None, 'col')
- w_x2: bfloat16 [2, 4096, 16384], P(None, 'row', 'col')
- w_h2: bfloat16 [4096, 16384], P('row', 'col')
- b_2: float32 [16384], P('col')
- h_zero: float32 [3, 64, 4096], P(None, 'data', 'row'), parts along dimension 1
- c_zero: float32 [3, 64, 4096], P(None, 'data', 'row'), parts along dimension 1
Outputs:
- output 1: bfloat16 [16, 64, 4096], P(None, 'data', ('col', 'row')), parts along dimension 1
- output 2: float32 [3, 64, 4096], P(None, 'data', ('col', 'row')), parts along dimension 1
There are 2 independent parts. The reference program is written for one: setup_inputs(seed, part) draws one part's arguments, and reference() takes and returns one part's arrays. A program takes and returns all parts, laid end to end along the dimension named above; an argument that names none is the same for every part.
All inputs are finite; a program needn't handle non-finite values.
Results may differ from the reference program's by a relative error of at most 0.00315333.
Values are sent between devices in bfloat16 or wider.
A program may use at most 1 GiB of HBM per device.

```python
import jax
import jax.numpy as jnp
from jax import lax

STEPS = 16
BATCH = 32
D = 4096


def setup_inputs(seed: int = 0, part: int = 0) -> dict:
    key = jax.random.key(seed)
    shared = jax.random.split(key, 6)
    own = jax.random.split(jax.random.fold_in(key, part), 3)
    in_scale = D ** -0.5
    x = jax.random.normal(own[0], (STEPS, BATCH, D), jnp.float32)
    w_x1 = jax.random.normal(shared[0], (2, D, 4 * D), jnp.float32) * in_scale
    w_h1 = jax.random.normal(shared[1], (2, D, 4 * D), jnp.float32) * in_scale
    b_1 = 0.5 * jax.random.normal(shared[2], (2, 4 * D), jnp.float32)
    w_x2 = jax.random.normal(shared[3], (2, D, 4 * D), jnp.float32) * in_scale
    w_h2 = jax.random.normal(shared[4], (D, 4 * D), jnp.float32) * in_scale
    b_2 = 0.5 * jax.random.normal(shared[5], (4 * D,), jnp.float32)
    h_zero = 0.9 * jnp.tanh(jax.random.normal(own[1], (3, BATCH, D), jnp.float32))
    c_zero = 1.5 * jax.random.normal(own[2], (3, BATCH, D), jnp.float32)
    return {'x': x.astype(jnp.bfloat16), 'w_x1': w_x1.astype(jnp.bfloat16),
            'w_h1': w_h1.astype(jnp.bfloat16), 'b_1': b_1,
            'w_x2': w_x2.astype(jnp.bfloat16), 'w_h2': w_h2.astype(jnp.bfloat16),
            'b_2': b_2, 'h_zero': h_zero, 'c_zero': c_zero}


def lstm_layer(in_seq, w_in, w_rec, gate_bias, h_init, c_init, backward):
    def one_step(carry, in_t):
        h_prev, c_prev = carry
        z_all = (jnp.dot(in_t, w_in, preferred_element_type=jnp.float32)
                 + jnp.dot(h_prev, w_rec, preferred_element_type=jnp.float32) + gate_bias)
        gates = z_all.reshape(z_all.shape[0], D, 4)
        c_next = (jax.nn.sigmoid(gates[:, :, 1]) * c_prev
                  + jax.nn.sigmoid(gates[:, :, 0]) * jnp.tanh(gates[:, :, 2]))
        h_next = (jax.nn.sigmoid(gates[:, :, 3]) * jnp.tanh(c_next)).astype(jnp.bfloat16)
        return (h_next, c_next), h_next
    carry_out, h_seq = lax.scan(one_step, (h_init.astype(jnp.bfloat16), c_init), in_seq, reverse=backward)
    return h_seq, carry_out[1]


def reference(x, w_x1, w_h1, b_1, w_x2, w_h2, b_2, h_zero, c_zero):
    fwd_seq, fwd_cell = lstm_layer(x, w_x1[0], w_h1[0], b_1[0], h_zero[0], c_zero[0], False)
    bwd_seq, bwd_cell = lstm_layer(x, w_x1[1], w_h1[1], b_1[1], h_zero[1], c_zero[1], True)
    mid_seq = jnp.concatenate([fwd_seq, bwd_seq], axis=2)
    top_seq, top_cell = lstm_layer(mid_seq, w_x2.reshape(2 * D, 4 * D), w_h2, b_2,
                                   h_zero[2], c_zero[2], False)
    return top_seq, jnp.stack([fwd_cell, bwd_cell, top_cell])
```

```python
import functools

import jax
import jax.numpy as jnp
from jax import lax
from jax.experimental import pallas as pl
from jax.experimental.pallas import tpu as pltpu
from jax.sharding import PartitionSpec as P

MESH = pl.DeviceIdType.MESH
F32 = jnp.float32
BF16 = jnp.bfloat16
LANES = 128


def lstm_kernel(steps, n_row, n_col,
                x_ref, wx1_hbm, wh1_hbm, wx2_hbm, wh2_hbm, b1_ref, b2_ref, h0_ref, c0_ref,
                out_ref, c_ref,
                wx, wh, wh2, hist, h2b, zp, p1r, yr, hsend, sel,
                w_sem, p1_send, p1_recv, y_send, y_recv, h_send, h_recv):
    row = lax.axis_index('row')
    col = lax.axis_index('col')
    batch, d_row = x_ref.shape[1], x_ref.shape[2]
    unit_n = d_row // n_col
    width = 4 * unit_n
    core = row % 2
    mate = row + 1 - 2 * core
    across = (row + 2) % 4
    order = (3 - row, across, mate, row)

    def weight_copy(src, dst, idx, sem):
        cols = pl.ds(pl.multiple_of(order[idx] * width, LANES), width)
        return pltpu.make_async_copy(src.at[:, cols], dst.at[idx], w_sem.at[sem, idx])

    loads = {'x0': (wx1_hbm.at[0], wx.at[0], 0), 'h0': (wh1_hbm.at[0], wh.at[0], 1),
             'x1': (wx1_hbm.at[1], wx.at[1], 2), 'h1': (wh1_hbm.at[1], wh.at[1], 3),
             'h2': (wh2_hbm, wh2, 4),
             'm0': (wx2_hbm.at[0], wx.at[0], 5), 'm1': (wx2_hbm.at[1], wx.at[1], 6)}

    def load_start(name):
        for idx in range(4):
            src, dst, sem = loads[name]
            weight_copy(src, dst, idx, sem).start()

    def load_wait(name):
        for idx in range(4):
            src, dst, sem = loads[name]
            weight_copy(src, dst, idx, sem).wait()

    for name in ('x0', 'h0', 'x1', 'h1', 'h2'):
        load_start(name)

    barrier = pltpu.get_barrier_semaphore()
    for dc in range(n_col):
        for dr in range(n_row):
            if dc or dr:
                pl.semaphore_signal(barrier, inc=1, device_id_type=MESH,
                                    device_id={'col': (col + dc) % n_col, 'row': (row + dr) % n_row})

    rr = lax.broadcasted_iota(jnp.int32, (width, unit_n), 0)
    cc = lax.broadcasted_iota(jnp.int32, (width, unit_n), 1)
    sel[...] = jnp.where(rr == 4 * cc, 1.0, 0.0).astype(BF16)
    for k in range(2):
        for j in range(n_row):
            hist[k, 0, j] = h0_ref[k, :, j * unit_n:(j + 1) * unit_n].astype(BF16)
    for j in range(n_row):
        h2b[0, j] = h0_ref[2, :, j * unit_n:(j + 1) * unit_n].astype(BF16)
    c_ref[...] = c0_ref[...]

    def dot(a, w):
        return jnp.dot(a, w, preferred_element_type=F32)

    def joined(blocks):
        return jnp.concatenate([blocks[j] for j in range(n_row)], axis=1)

    def input_product(k, t):
        a = x_ref[t]
        for idx in range(4):
            zp[k, idx] = dot(a, wx[k, idx])

    load_wait('x0')
    input_product(0, 0)
    load_wait('x1')
    input_product(1, steps - 1)
    load_wait('h0')
    load_wait('h1')
    pl.semaphore_wait(barrier, n_col * n_row - 1)

    def mate_copy(k, slot, part):
        return pltpu.make_async_remote_copy(
            src_ref=zp.at[k, 2 * part], dst_ref=p1r.at[k, slot, part],
            send_sem=p1_send.at[k, part], recv_sem=p1_recv.at[k, slot, part],
            device_id={'row': mate}, device_id_type=MESH)

    def across_copy(k, slot):
        return pltpu.make_async_remote_copy(
            src_ref=zp.at[k, 1], dst_ref=yr.at[k, slot],
            send_sem=y_send.at[k], recv_sem=y_recv.at[k, slot],
            device_id={'row': across}, device_id_type=MESH)

    def h_copy(k, dst, slot, i):
        return pltpu.make_async_remote_copy(
            src_ref=hsend.at[k], dst_ref=dst.at[row],
            send_sem=h_send.at[k, i], recv_sem=h_recv.at[k, slot, row],
            device_id={'col': (col + i) % n_col, 'row': col}, device_id_type=MESH)

    own_stays = row == col

    def h_start(k, dst, slot):
        for i in range(n_col - 1, 0, -1):
            h_copy(k, dst, slot, i).start()

        @pl.when(jnp.logical_not(own_stays))
        def _():
            h_copy(k, dst, slot, 0).start()

        @pl.when(own_stays)
        def _():
            dst[row] = hsend[k]

    def h_wait_send(k, dst, slot):
        for i in range(1, n_col):
            h_copy(k, dst, slot, i).wait_send()

        @pl.when(jnp.logical_not(own_stays))
        def _():
            h_copy(k, dst, slot, 0).wait_send()

    def h_wait_recv(k, dst, slot):
        for j in range(n_row):
            def wait(j=j):
                pltpu.make_async_remote_copy(
                    src_ref=hsend.at[k], dst_ref=dst.at[j],
                    send_sem=h_send.at[k, 0], recv_sem=h_recv.at[k, slot, j],
                    device_id={'col': col, 'row': row}, device_id_type=MESH).wait_recv()
            pl.when(jnp.logical_not(own_stays & (row == j)))(wait)

    def head(k, slot, blocks, w_rec):
        a = joined(blocks)
        for idx in range(4):
            zp[k, idx] = zp[k, idx] + dot(a, w_rec[idx])
            if idx % 2 == 0:
                mate_copy(k, slot, idx // 2).start()

    def middle(k, slot):
        mate_copy(k, slot, 0).wait_recv()
        zp[k, 1] = zp[k, 1] + p1r[k, slot, 0]
        across_copy(k, slot).start()

    def gates(k, slot, cell, bias_ref, bias_row):
        mate_copy(k, slot, 1).wait_recv()
        across_copy(k, slot).wait_recv()
        gate = lax.broadcasted_iota(jnp.int32, (batch, LANES), 1) % 4
        scale = jnp.where(gate == 2, 1.0, 0.5)
        shift = jnp.where(gate == 2, 0.0, 0.5)
        pieces = []
        for p in range(width // LANES):
            lanes = slice(p * LANES, (p + 1) * LANES)
            bias = bias_ref[bias_row:bias_row + 1, pl.ds(pl.multiple_of(row * width, LANES) + p * LANES, LANES)]
            z = zp[k, 3, :, lanes] + p1r[k, slot, 1, :, lanes] + yr[k, slot, :, lanes] + bias
            act = jnp.tanh(z * scale) * scale + shift
            f = pltpu.roll(act, LANES - 1, 1)
            g = pltpu.roll(act, LANES - 2, 1)
            o = pltpu.roll(act, LANES - 3, 1)
            c_new = f * c_ref[cell, :, lanes] + act * g
            c_ref[cell, :, lanes] = c_new
            pieces.append((o * jnp.tanh(c_new)).astype(BF16))
        h = dot(jnp.concatenate(pieces, axis=1), sel[...]).astype(BF16)
        for part in range(2):
            mate_copy(k, slot, part).wait_send()
        across_copy(k, slot).wait_send()
        return h

    def layer_one(n, carry):
        slot = n % 2
        for k in range(2):
            @pl.when(n > 0)
            def _(k=k):
                h_wait_recv(k, hist.at[k, n], slot)
            head(k, slot, hist.at[k, n], wh.at[k])
            middle(k, slot)
        for k in range(2):
            h = gates(k, slot, k, b1_ref, k)

            @pl.when(n > 0)
            def _(k=k):
                h_wait_send(k, hist.at[k, n], slot)
            hsend[k] = h
            h_start(k, hist.at[k, n + 1], (n + 1) % 2)

            @pl.when(n < steps - 1)
            def _(k=k):
                input_product(k, n + 1 if k == 0 else steps - 2 - n)

            @pl.when(n == steps - 1)
            def _(k=k):
                load_start('m0' if k == 0 else 'm1')
        return carry

    lax.fori_loop(0, steps, layer_one, 0)

    def mid_product(t):
        a = joined(hist.at[0, t + 1])
        b = joined(hist.at[1, steps - t])
        for idx in range(4):
            zp[0, idx] = dot(a, wx[0, idx]) + dot(b, wx[1, idx])

    for k in range(2):
        h_wait_send(k, hist.at[k, steps], steps % 2)
    for name in ('h2', 'm0', 'm1'):
        load_wait(name)
    for k in range(2):
        h_wait_recv(k, hist.at[k, steps], steps % 2)
    mid_product(0)

    def layer_two(n, carry):
        slot = n % 2

        @pl.when(n > 0)
        def _():
            h_wait_recv(2, h2b.at[slot], slot)
        head(0, slot, h2b.at[slot], wh2)
        middle(0, slot)
        h = gates(0, slot, 2, b2_ref, 0)

        @pl.when(n > 0)
        def _():
            h_wait_send(2, h2b.at[slot], slot)
        hsend[2] = h
        out_ref[n] = h

        @pl.when(n < steps - 1)
        def _():
            h_start(2, h2b.at[1 - slot], 1 - slot)
            mid_product(n + 1)
        return carry

    lax.fori_loop(0, steps, layer_two, 0)


def solution(mesh):
    n_row = mesh.shape['row']
    n_col = mesh.shape['col']
    spec_seq = P(None, 'data', 'row')
    spec_weight = P(None, 'row', 'col')
    spec_out = P(None, 'data', ('col', 'row'))

    def local(x_rows, w_x1, w_h1, b_1, w_x2, w_h2, b_2, h_zero, c_zero):
        row_idx = lax.axis_index('row')
        col_idx = lax.axis_index('col')
        steps, batch, d_row = x_rows.shape
        unit_n = d_row // n_col
        width = 4 * unit_n
        c_part = lax.dynamic_slice_in_dim(c_zero, col_idx * unit_n, unit_n, axis=2)
        pairs = [(b * n_row + a, a * n_row + b) for a in range(n_row) for b in range(n_col)]
        c_own = lax.ppermute(c_part, ('col', 'row'), pairs)
        c_wide = jnp.repeat(c_own, 4, axis=2)
        vmem = pl.BlockSpec(memory_space=pltpu.VMEM)
        hbm = pl.BlockSpec(memory_space=pl.ANY)
        dma = pltpu.SemaphoreType.DMA
        out, c_out = pl.pallas_call(
            functools.partial(lstm_kernel, steps, n_row, n_col),
            out_shape=(jax.ShapeDtypeStruct((steps, batch, unit_n), BF16),
                       jax.ShapeDtypeStruct((3, batch, width), F32)),
            in_specs=[vmem, hbm, hbm, hbm, hbm, vmem, vmem, vmem, vmem],
            out_specs=(vmem, vmem),
            scratch_shapes=[
                pltpu.VMEM((2, 4, d_row, width), BF16),
                pltpu.VMEM((2, 4, d_row, width), BF16),
                pltpu.VMEM((4, d_row, width), BF16),
                pltpu.VMEM((2, steps + 1, n_row, batch, unit_n), BF16),
                pltpu.VMEM((2, n_row, batch, unit_n), BF16),
                pltpu.VMEM((2, 4, batch, width), F32),
                pltpu.VMEM((2, 2, 2, batch, width), F32),
                pltpu.VMEM((2, 2, batch, width), F32),
                pltpu.VMEM((3, batch, unit_n), BF16),
                pltpu.VMEM((width, unit_n), BF16),
                dma((7, 4)), dma((2, 2)), dma((2, 2, 2)), dma((2,)), dma((2, 2)),
                dma((3, n_col)), dma((3, 2, n_row)),
            ],
            compiler_params=pltpu.CompilerParams(
                collective_id=0, has_side_effects=True, vmem_limit_bytes=60 * 1024 * 1024),
        )(x_rows, w_x1, w_h1, w_x2, w_h2, b_1, b_2[None], h_zero, c_wide)
        return out, c_out[:, :, ::4]

    return jax.shard_map(local, mesh=mesh,
                         in_specs=(spec_seq, spec_weight, spec_weight, P(None, 'col'), spec_weight,
                                   P('row', 'col'), P('col'), spec_seq, spec_seq),
                         out_specs=(spec_out, spec_out), check_vma=False)
```

```python
import functools

import jax
import jax.numpy as jnp
from jax import lax
from jax.experimental import pallas as pl
from jax.experimental.pallas import tpu as pltpu
from jax.sharding import PartitionSpec as P

MESH = pl.DeviceIdType.MESH
F32 = jnp.float32
BF16 = jnp.bfloat16
LANES = 128


def lstm_kernel(steps, n_row, n_col,
                x_ref, wx1_hbm, wh1_hbm, wx2_hbm, wh2_hbm, b1_ref, b2_ref, h0_ref, c0_ref,
                out_ref, c_out,
                wx, wh, wh2, hist, h2b, zp, p1r, yr, hsend, sel, spread, c_own, c_ref,
                c_sem, w_sem, p1_send, p1_recv, y_send, y_recv, h_send, h_recv):
    row = lax.axis_index('row')
    col = lax.axis_index('col')
    batch, d_row = x_ref.shape[1], x_ref.shape[2]
    unit_n = d_row // n_col
    width = 4 * unit_n
    core = row % 2
    mate = row + 1 - 2 * core
    across = (row + 2) % 4
    order = (3 - row, across, mate, row)

    def weight_copy(src, dst, idx, sem):
        cols = pl.ds(pl.multiple_of(order[idx] * width, LANES), width)
        return pltpu.make_async_copy(src.at[:, cols], dst.at[idx], w_sem.at[sem, idx])

    loads = {'x0': (wx1_hbm.at[0], wx.at[0], 0), 'h0': (wh1_hbm.at[0], wh.at[0], 1),
             'x1': (wx1_hbm.at[1], wx.at[1], 2), 'h1': (wh1_hbm.at[1], wh.at[1], 3),
             'h2': (wh2_hbm, wh2, 4),
             'm0': (wx2_hbm.at[0], wx.at[0], 5), 'm1': (wx2_hbm.at[1], wx.at[1], 6)}

    def load_start(name):
        for idx in range(4):
            src, dst, sem = loads[name]
            weight_copy(src, dst, idx, sem).start()

    def load_wait(name):
        for idx in range(4):
            src, dst, sem = loads[name]
            weight_copy(src, dst, idx, sem).wait()

    for name in ('x0', 'h0', 'x1', 'h1', 'h2'):
        load_start(name)

    barrier = pltpu.get_barrier_semaphore()
    for dc in range(n_col):
        for dr in range(n_row):
            if dc or dr:
                pl.semaphore_signal(barrier, inc=1, device_id_type=MESH,
                                    device_id={'col': (col + dc) % n_col, 'row': (row + dr) % n_row})

    rr = lax.broadcasted_iota(jnp.int32, (width, unit_n), 0)
    cc = lax.broadcasted_iota(jnp.int32, (width, unit_n), 1)
    sel[...] = jnp.where(rr == 4 * cc, 1.0, 0.0).astype(BF16)
    for k in range(2):
        for j in range(n_row):
            hist[k, 0, j] = h0_ref[k, :, j * unit_n:(j + 1) * unit_n].astype(BF16)
    for j in range(n_row):
        h2b[0, j] = h0_ref[2, :, j * unit_n:(j + 1) * unit_n].astype(BF16)
    rr = lax.broadcasted_iota(jnp.int32, (unit_n, width), 0)
    cc = lax.broadcasted_iota(jnp.int32, (unit_n, width), 1)
    spread[...] = jnp.where(rr == cc // 4, 1.0, 0.0).astype(BF16)

    own_stays = row == col
    c_part = pl.ds(pl.multiple_of(col * unit_n, LANES), unit_n)
    c_copy = pltpu.make_async_remote_copy(
        src_ref=c0_ref.at[:, :, c_part], dst_ref=c_own, send_sem=c_sem.at[0], recv_sem=c_sem.at[1],
        device_id={'col': row, 'row': col}, device_id_type=MESH)
    pl.semaphore_wait(barrier, n_col * n_row - 1)

    @pl.when(jnp.logical_not(own_stays))
    def _():
        c_copy.start()

    @pl.when(own_stays)
    def _():
        c_own[...] = c0_ref[:, :, c_part]

    def dot(a, w):
        return jnp.dot(a, w, preferred_element_type=F32)

    def moved(a, m):
        a = a * 0.5
        top = a.astype(BF16)
        rest = a - top.astype(F32)
        mid = rest.astype(BF16)
        low = (rest - mid.astype(F32)).astype(BF16)
        return (dot(top, m) + dot(mid, m) + dot(low, m)) * 2.0

    def joined(blocks):
        return jnp.concatenate([blocks[j] for j in range(n_row)], axis=1)

    def input_product(k, t):
        a = x_ref[t]
        for idx in range(4):
            zp[k, idx] = dot(a, wx[k, idx])

    load_wait('x0')
    input_product(0, 0)
    load_wait('x1')
    input_product(1, steps - 1)
    load_wait('h0')
    load_wait('h1')

    @pl.when(jnp.logical_not(own_stays))
    def _():
        c_copy.wait()
    for k in range(3):
        c_ref[k] = moved(c_own[k], spread[...])

    def mate_copy(k, slot, part):
        return pltpu.make_async_remote_copy(
            src_ref=zp.at[k, 2 * part], dst_ref=p1r.at[k, slot, part],
            send_sem=p1_send.at[k, part], recv_sem=p1_recv.at[k, slot, part],
            device_id={'row': mate}, device_id_type=MESH)

    def across_copy(k, slot):
        return pltpu.make_async_remote_copy(
            src_ref=zp.at[k, 1], dst_ref=yr.at[k, slot],
            send_sem=y_send.at[k], recv_sem=y_recv.at[k, slot],
            device_id={'row': across}, device_id_type=MESH)

    def h_copy(k, dst, slot, i):
        return pltpu.make_async_remote_copy(
            src_ref=hsend.at[k], dst_ref=dst.at[row],
            send_sem=h_send.at[k, i], recv_sem=h_recv.at[k, slot, row],
            device_id={'col': (col + i) % n_col, 'row': col}, device_id_type=MESH)

    def h_start(k, dst, slot):
        for i in range(n_col - 1, 0, -1):
            h_copy(k, dst, slot, i).start()

        @pl.when(jnp.logical_not(own_stays))
        def _():
            h_copy(k, dst, slot, 0).start()

        @pl.when(own_stays)
        def _():
            dst[row] = hsend[k]

    def h_wait_send(k, dst, slot):
        for i in range(1, n_col):
            h_copy(k, dst, slot, i).wait_send()

        @pl.when(jnp.logical_not(own_stays))
        def _():
            h_copy(k, dst, slot, 0).wait_send()

    def h_wait_recv(k, dst, slot):
        for j in range(n_row):
            def wait(j=j):
                pltpu.make_async_remote_copy(
                    src_ref=hsend.at[k], dst_ref=dst.at[j],
                    send_sem=h_send.at[k, 0], recv_sem=h_recv.at[k, slot, j],
                    device_id={'col': col, 'row': row}, device_id_type=MESH).wait_recv()
            pl.when(jnp.logical_not(own_stays & (row == j)))(wait)

    def head(k, slot, blocks, w_rec):
        a = joined(blocks)
        for idx in range(4):
            zp[k, idx] = zp[k, idx] + dot(a, w_rec[idx])
            if idx % 2 == 0:
                mate_copy(k, slot, idx // 2).start()

    def middle(k, slot):
        mate_copy(k, slot, 0).wait_recv()
        zp[k, 1] = zp[k, 1] + p1r[k, slot, 0]
        across_copy(k, slot).start()

    def gates(k, slot, cell, bias_ref, bias_row):
        mate_copy(k, slot, 1).wait_recv()
        across_copy(k, slot).wait_recv()
        gate = lax.broadcasted_iota(jnp.int32, (batch, LANES), 1) % 4
        scale = jnp.where(gate == 2, 1.0, 0.5)
        shift = jnp.where(gate == 2, 0.0, 0.5)
        pieces = []
        for p in range(width // LANES):
            lanes = slice(p * LANES, (p + 1) * LANES)
            bias = bias_ref[bias_row:bias_row + 1, pl.ds(pl.multiple_of(row * width, LANES) + p * LANES, LANES)]
            z = zp[k, 3, :, lanes] + p1r[k, slot, 1, :, lanes] + yr[k, slot, :, lanes] + bias
            act = jnp.tanh(z * scale) * scale + shift
            f = pltpu.roll(act, LANES - 1, 1)
            g = pltpu.roll(act, LANES - 2, 1)
            o = pltpu.roll(act, LANES - 3, 1)
            c_new = f * c_ref[cell, :, lanes] + act * g
            c_ref[cell, :, lanes] = c_new
            pieces.append((o * jnp.tanh(c_new)).astype(BF16))
        h = dot(jnp.concatenate(pieces, axis=1), sel[...]).astype(BF16)
        for part in range(2):
            mate_copy(k, slot, part).wait_send()
        across_copy(k, slot).wait_send()
        return h

    def layer_one(n, carry):
        slot = n % 2
        for k in range(2):
            @pl.when(n > 0)
            def _(k=k):
                h_wait_recv(k, hist.at[k, n], slot)
            head(k, slot, hist.at[k, n], wh.at[k])
            middle(k, slot)
        for k in range(2):
            h = gates(k, slot, k, b1_ref, k)

            @pl.when(n > 0)
            def _(k=k):
                h_wait_send(k, hist.at[k, n], slot)
            hsend[k] = h
            h_start(k, hist.at[k, n + 1], (n + 1) % 2)

            @pl.when(n < steps - 1)
            def _(k=k):
                input_product(k, n + 1 if k == 0 else steps - 2 - n)

            @pl.when(n == steps - 1)
            def _(k=k):
                load_start('m0' if k == 0 else 'm1')
        return carry

    lax.fori_loop(0, steps, layer_one, 0)

    def mid_product(t):
        a = joined(hist.at[0, t + 1])
        b = joined(hist.at[1, steps - t])
        for idx in range(4):
            zp[0, idx] = dot(a, wx[0, idx]) + dot(b, wx[1, idx])

    for k in range(2):
        h_wait_send(k, hist.at[k, steps], steps % 2)
    for name in ('h2', 'm0', 'm1'):
        load_wait(name)
    for k in range(2):
        h_wait_recv(k, hist.at[k, steps], steps % 2)
    mid_product(0)

    def layer_two(n, carry):
        slot = n % 2

        @pl.when(n > 0)
        def _():
            h_wait_recv(2, h2b.at[slot], slot)
        head(0, slot, h2b.at[slot], wh2)
        middle(0, slot)
        h = gates(0, slot, 2, b2_ref, 0)

        @pl.when(n > 0)
        def _():
            h_wait_send(2, h2b.at[slot], slot)
        hsend[2] = h
        out_ref[n] = h

        @pl.when(n < steps - 1)
        def _():
            h_start(2, h2b.at[1 - slot], 1 - slot)
            mid_product(n + 1)
        return carry

    lax.fori_loop(0, steps, layer_two, 0)
    for k in range(3):
        c_out[k] = moved(c_ref[k], sel[...])


def solution(mesh):
    n_row = mesh.shape['row']
    n_col = mesh.shape['col']
    spec_seq = P(None, 'data', 'row')
    spec_weight = P(None, 'row', 'col')
    spec_out = P(None, 'data', ('col', 'row'))

    def local(x_rows, w_x1, w_h1, b_1, w_x2, w_h2, b_2, h_zero, c_zero):
        steps, batch, d_row = x_rows.shape
        unit_n = d_row // n_col
        width = 4 * unit_n
        vmem = pl.BlockSpec(memory_space=pltpu.VMEM)
        hbm = pl.BlockSpec(memory_space=pl.ANY)
        dma = pltpu.SemaphoreType.DMA
        return pl.pallas_call(
            functools.partial(lstm_kernel, steps, n_row, n_col),
            out_shape=(jax.ShapeDtypeStruct((steps, batch, unit_n), BF16),
                       jax.ShapeDtypeStruct((3, batch, unit_n), F32)),
            in_specs=[vmem, hbm, hbm, hbm, hbm, vmem, vmem, vmem, vmem],
            out_specs=(vmem, vmem),
            scratch_shapes=[
                pltpu.VMEM((2, 4, d_row, width), BF16),
                pltpu.VMEM((2, 4, d_row, width), BF16),
                pltpu.VMEM((4, d_row, width), BF16),
                pltpu.VMEM((2, steps + 1, n_row, batch, unit_n), BF16),
                pltpu.VMEM((2, n_row, batch, unit_n), BF16),
                pltpu.VMEM((2, 4, batch, width), F32),
                pltpu.VMEM((2, 2, 2, batch, width), F32),
                pltpu.VMEM((2, 2, batch, width), F32),
                pltpu.VMEM((3, batch, unit_n), BF16),
                pltpu.VMEM((width, unit_n), BF16),
                pltpu.VMEM((unit_n, width), BF16),
                pltpu.VMEM((3, batch, unit_n), F32),
                pltpu.VMEM((3, batch, width), F32),
                dma((2,)),
                dma((7, 4)), dma((2, 2)), dma((2, 2, 2)), dma((2,)), dma((2, 2)),
                dma((3, n_col)), dma((3, 2, n_row)),
            ],
            compiler_params=pltpu.CompilerParams(
                collective_id=0, has_side_effects=True, vmem_limit_bytes=60 * 1024 * 1024),
        )(x_rows, w_x1, w_h1, w_x2, w_h2, b_1, b_2[None], h_zero, c_zero)

    return jax.shard_map(local, mesh=mesh,
                         in_specs=(spec_seq, spec_weight, spec_weight, P(None, 'col'), spec_weight,
                                   P('row', 'col'), P('col'), spec_seq, spec_seq),
                         out_specs=(spec_out, spec_out), check_vma=False)
```

```python
import functools

import jax
import jax.numpy as jnp
from jax import lax
from jax.experimental import pallas as pl
from jax.experimental.pallas import tpu as pltpu
from jax.sharding import PartitionSpec as P

MESH = pl.DeviceIdType.MESH
F32 = jnp.float32
BF16 = jnp.bfloat16
LANES = 128


def lstm_kernel(steps, n_data, n_row, n_col,
                x_ref, wx1_hbm, wh1_hbm, wx2_hbm, wh2_hbm, b1_ref, b2_ref, h0_ref, c0_ref,
                out_ref, c_out,
                wx, wh, wh2, hist, h2b, zp, p1r, yr, zm, m1r, myr, hsend, sel, spread, c_own, c_ref,
                c_sem, w_sem, p1_send, p1_recv, y_send, y_recv, m1_send, m1_recv, my_send, my_recv,
                h_send, h_recv, h2_send, h2_recv, h0_sem, move_send, move_recv, relay_send, relay_recv):
    data = lax.axis_index('data')
    row = lax.axis_index('row')
    col = lax.axis_index('col')
    batch, d_row = x_ref.shape[1], x_ref.shape[2]
    unit_n = d_row // n_col
    width = 4 * unit_n
    core = row % 2
    mate = row + 1 - 2 * core
    across = (row + 2) % 4
    order = (3 - row, across, mate, row)

    def weight_copy(src, dst, idx, sem):
        cols = pl.ds(pl.multiple_of(order[idx] * width, LANES), width)
        return pltpu.make_async_copy(src.at[:, cols], dst.at[idx], w_sem.at[sem, idx])

    loads = {'x0': (wx1_hbm.at[0], wx.at[0], 0), 'h0': (wh1_hbm.at[0], wh.at[0], 1),
             'x1': (wx1_hbm.at[1], wx.at[1], 2), 'h1': (wh1_hbm.at[1], wh.at[1], 3),
             'm0': (wx2_hbm.at[0], wx.at[0], 4), 'm1': (wx2_hbm.at[1], wx.at[1], 5)}

    def load_start(name):
        for idx in range(4):
            src, dst, sem = loads[name]
            weight_copy(src, dst, idx, sem).start()

    def load_wait(name):
        for idx in range(4):
            src, dst, sem = loads[name]
            weight_copy(src, dst, idx, sem).wait()

    for name in ('x0', 'h0', 'x1', 'h1'):
        load_start(name)

    half = d_row // 2
    piece = half // (2 * steps)
    own_cols = pl.ds(pl.multiple_of(row // 2 * (2 * width), LANES), 2 * width)
    far_cols = pl.ds(pl.multiple_of((1 - row // 2) * (2 * width), LANES), 2 * width)
    h2_load = pltpu.make_async_copy(wh2_hbm.at[:, own_cols], wh2.at[0], w_sem.at[6, 0])
    h2_load.start()

    def piece_rows(part, p):
        return pl.ds(pl.multiple_of(part * half + p * piece, 16), piece)

    def move_copy(p):
        rows = piece_rows(data, p)
        return pltpu.make_async_remote_copy(
            src_ref=wh2_hbm.at[rows, far_cols], dst_ref=wh2.at[1, rows],
            send_sem=move_send, recv_sem=move_recv.at[p % 8],
            device_id={'row': across}, device_id_type=MESH)

    def relay_copy(p):
        rows = piece_rows(data, p)
        return pltpu.make_async_remote_copy(
            src_ref=wh2.at[1, rows], dst_ref=wh2.at[1, rows],
            send_sem=relay_send, recv_sem=relay_recv,
            device_id={'data': 1 - data}, device_id_type=MESH)

    def forward(p):
        move_copy(p).wait_recv()
        relay_copy(p).start()

    barrier = pltpu.get_barrier_semaphore()
    for dc in range(n_col):
        for dr in range(n_row):
            if dc or dr:
                pl.semaphore_signal(barrier, inc=1, device_id_type=MESH,
                                    device_id={'col': (col + dc) % n_col, 'row': (row + dr) % n_row})
    pl.semaphore_signal(barrier, inc=1, device_id_type=MESH, device_id={'data': 1 - data})

    rr = lax.broadcasted_iota(jnp.int32, (width, unit_n), 0)
    cc = lax.broadcasted_iota(jnp.int32, (width, unit_n), 1)
    sel[...] = jnp.where(rr == 4 * cc, 1.0, 0.0).astype(BF16)
    for k in range(2):
        for j in range(n_row):
            hist[k, 0, j] = h0_ref[k, :, j * unit_n:(j + 1) * unit_n].astype(BF16)
    for j in range(n_row):
        h2b[0, 0, j] = h0_ref[2, :, j * unit_n:(j + 1) * unit_n].astype(BF16)
    rr = lax.broadcasted_iota(jnp.int32, (unit_n, width), 0)
    cc = lax.broadcasted_iota(jnp.int32, (unit_n, width), 1)
    spread[...] = jnp.where(rr == cc // 4, 1.0, 0.0).astype(BF16)

    own_stays = row == col
    c_part = pl.ds(pl.multiple_of(col * unit_n, LANES), unit_n)
    c_copy = pltpu.make_async_remote_copy(
        src_ref=c0_ref.at[:, :, c_part], dst_ref=c_own, send_sem=c_sem.at[0], recv_sem=c_sem.at[1],
        device_id={'col': row, 'row': col}, device_id_type=MESH)
    pl.semaphore_wait(barrier, n_col * n_row)

    @pl.when(jnp.logical_not(own_stays))
    def _():
        c_copy.start()

    @pl.when(own_stays)
    def _():
        c_own[...] = c0_ref[:, :, c_part]

    h0_copy = pltpu.make_async_remote_copy(
        src_ref=h2b.at[0, 0], dst_ref=h2b.at[0, 1], send_sem=h0_sem.at[0], recv_sem=h0_sem.at[1],
        device_id={'row': across}, device_id_type=MESH)
    h0_copy.start()

    def dot(a, w):
        return jnp.dot(a, w, preferred_element_type=F32)

    def moved(a, m):
        a = a * 0.5
        top = a.astype(BF16)
        rest = a - top.astype(F32)
        mid = rest.astype(BF16)
        low = (rest - mid.astype(F32)).astype(BF16)
        parts = dot(jnp.concatenate([top, mid, low], axis=0), m)
        return ((parts[:batch] + parts[batch:2 * batch]) + parts[2 * batch:]) * 2.0

    def joined(blocks):
        return jnp.concatenate([blocks[j] for j in range(n_row)], axis=1)

    def input_product(k, t):
        a = x_ref[t]
        for idx in range(4):
            zp[k, idx] = dot(a, wx[k, idx])

    load_wait('x0')
    input_product(0, 0)
    load_wait('x1')
    input_product(1, steps - 1)
    load_wait('h0')
    load_wait('h1')

    @pl.when(jnp.logical_not(own_stays))
    def _():
        c_copy.wait()
    for k in range(3):
        c_ref[k] = moved(c_own[k], spread[...])

    def mate_copy(k, slot, part):
        return pltpu.make_async_remote_copy(
            src_ref=zp.at[k, 2 * part], dst_ref=p1r.at[k, slot, part],
            send_sem=p1_send.at[k, part], recv_sem=p1_recv.at[k, slot, part],
            device_id={'row': mate}, device_id_type=MESH)

    def across_copy(k, slot):
        return pltpu.make_async_remote_copy(
            src_ref=zp.at[k, 1], dst_ref=yr.at[k, slot],
            send_sem=y_send.at[k], recv_sem=y_recv.at[k, slot],
            device_id={'row': across}, device_id_type=MESH)

    def h_copy(k, dst, slot, i):
        return pltpu.make_async_remote_copy(
            src_ref=hsend.at[k], dst_ref=dst.at[row],
            send_sem=h_send.at[k, i], recv_sem=h_recv.at[k, slot, row],
            device_id={'col': (col + i) % n_col, 'row': col}, device_id_type=MESH)

    def h_start(k, dst, slot):
        for i in range(n_col - 1, 0, -1):
            h_copy(k, dst, slot, i).start()

        @pl.when(jnp.logical_not(own_stays))
        def _():
            h_copy(k, dst, slot, 0).start()

        @pl.when(own_stays)
        def _():
            dst[row] = hsend[k]

    def h_wait_send(k, dst, slot):
        for i in range(1, n_col):
            h_copy(k, dst, slot, i).wait_send()

        @pl.when(jnp.logical_not(own_stays))
        def _():
            h_copy(k, dst, slot, 0).wait_send()

    def h_wait_recv(k, dst, slot):
        for j in range(n_row):
            def wait(j=j):
                pltpu.make_async_remote_copy(
                    src_ref=hsend.at[k], dst_ref=dst.at[j],
                    send_sem=h_send.at[k, 0], recv_sem=h_recv.at[k, slot, j],
                    device_id={'col': col, 'row': row}, device_id_type=MESH).wait_recv()
            pl.when(jnp.logical_not(own_stays & (row == j)))(wait)

    def head(k, slot, blocks, w_rec):
        a = joined(blocks)
        for idx in range(4):
            zp[k, idx] = zp[k, idx] + dot(a, w_rec[idx])
            if idx % 2 == 0:
                mate_copy(k, slot, idx // 2).start()

    def middle(k, slot):
        mate_copy(k, slot, 0).wait_recv()
        zp[k, 1] = zp[k, 1] + p1r[k, slot, 0]
        across_copy(k, slot).start()

    def gates(cell, bias_ref, bias_row, addends):
        gate = lax.broadcasted_iota(jnp.int32, (batch, LANES), 1) % 4
        scale = jnp.where(gate == 2, 1.0, 0.5)
        shift = jnp.where(gate == 2, 0.0, 0.5)
        pieces = []
        for p in range(width // LANES):
            lanes = slice(p * LANES, (p + 1) * LANES)
            z = bias_ref[bias_row:bias_row + 1, pl.ds(pl.multiple_of(row * width, LANES) + p * LANES, LANES)]
            for a in addends:
                z = z + a[:, lanes]
            act = jnp.tanh(z * scale) * scale + shift
            f = pltpu.roll(act, LANES - 1, 1)
            g = pltpu.roll(act, LANES - 2, 1)
            o = pltpu.roll(act, LANES - 3, 1)
            c_new = f * c_ref[cell, :, lanes] + act * g
            c_ref[cell, :, lanes] = c_new
            pieces.append((o * jnp.tanh(c_new)).astype(BF16))
        return dot(jnp.concatenate(pieces, axis=1), sel[...]).astype(BF16)

    def gates_one(k, slot):
        mate_copy(k, slot, 1).wait_recv()
        across_copy(k, slot).wait_recv()
        h = gates(k, b1_ref, k, (zp.at[k, 3], p1r.at[k, slot, 1], yr.at[k, slot]))
        for part in range(2):
            mate_copy(k, slot, part).wait_send()
        across_copy(k, slot).wait_send()
        return h

    def layer_one(n, carry):
        slot = n % 2
        for k in range(2):
            @pl.when(n > 0)
            def _(k=k):
                h_wait_recv(k, hist.at[k, n], slot)
            head(k, slot, hist.at[k, n], wh.at[k])
            middle(k, slot)
        for k in range(2):
            h = gates_one(k, slot)

            @pl.when(n > 0)
            def _(k=k):
                h_wait_send(k, hist.at[k, n], slot)
            hsend[k] = h
            h_start(k, hist.at[k, n + 1], (n + 1) % 2)
            move_copy(2 * n + k).start()

            @pl.when(n > 0)
            def _(k=k):
                forward(2 * n - 2 + k)

            @pl.when(n < steps - 1)
            def _(k=k):
                input_product(k, n + 1 if k == 0 else steps - 2 - n)

            @pl.when(n == steps - 1)
            def _(k=k):
                load_start('m0' if k == 0 else 'm1')
        return carry

    lax.fori_loop(0, steps, layer_one, 0)

    def mid_mate_copy(slot, part):
        return pltpu.make_async_remote_copy(
            src_ref=zp.at[1, 2 * part], dst_ref=m1r.at[slot, part],
            send_sem=m1_send.at[part], recv_sem=m1_recv.at[slot, part],
            device_id={'row': mate}, device_id_type=MESH)

    def mid_across_copy(slot):
        return pltpu.make_async_remote_copy(
            src_ref=zp.at[1, 1], dst_ref=myr.at[slot],
            send_sem=my_send, recv_sem=my_recv.at[slot],
            device_id={'row': across}, device_id_type=MESH)

    def mid_wait_send():
        for part in range(2):
            mid_mate_copy(0, part).wait_send()
        mid_across_copy(0).wait_send()

    def mid_product(t):
        slot = t % 3
        a = joined(hist.at[0, t + 1])
        b = joined(hist.at[1, steps - t])
        for idx in range(4):
            z = dot(a, wx[0, idx]) + dot(b, wx[1, idx])
            if idx < 3:
                zp[1, idx] = z
            else:
                zm[t % 2] = z
            if idx % 2 == 0:
                mid_mate_copy(slot, idx // 2).start()
        mid_mate_copy(slot, 0).wait_recv()
        zp[1, 1] = zp[1, 1] + m1r[slot, 0]
        mid_across_copy(slot).start()

    def h2_copy(slot, i, p):
        return pltpu.make_async_remote_copy(
            src_ref=hsend.at[2], dst_ref=h2b.at[slot, p, row],
            send_sem=h2_send.at[i, p], recv_sem=h2_recv.at[slot, p, row],
            device_id={'col': (col + i) % n_col, 'row': (col + 2 * p) % n_row}, device_id_type=MESH)

    h2_stays = [row == (col + 2 * p) % n_row for p in range(2)]

    def h2_start(slot):
        for i in range(n_col - 1, -1, -1):
            for p in range(2):
                if i:
                    h2_copy(slot, i, p).start()
                else:
                    pl.when(jnp.logical_not(h2_stays[p]))(lambda p=p: h2_copy(slot, 0, p).start())

                    @pl.when(h2_stays[p])
                    def _(p=p):
                        h2b[slot, p, row] = hsend[2]

    def h2_wait_send(slot):
        for i in range(n_col):
            for p in range(2):
                if i:
                    h2_copy(slot, i, p).wait_send()
                else:
                    pl.when(jnp.logical_not(h2_stays[p]))(lambda p=p: h2_copy(slot, 0, p).wait_send())

    def h2_wait_recv(slot):
        for p in range(2):
            for j in range(n_row):
                def wait(p=p, j=j):
                    pltpu.make_async_remote_copy(
                        src_ref=hsend.at[2], dst_ref=h2b.at[slot, p, j],
                        send_sem=h2_send.at[0, 0], recv_sem=h2_recv.at[slot, p, j],
                        device_id={'col': col, 'row': row}, device_id_type=MESH).wait_recv()
                pl.when(jnp.logical_not(h2_stays[p] & (row == j)))(wait)

    for k in range(2):
        forward(2 * steps - 2 + k)
    for k in range(2):
        h_wait_send(k, hist.at[k, steps], steps % 2)
    for name in ('m0', 'm1'):
        load_wait(name)
    mid_product(1)
    for k in range(2):
        h_wait_recv(k, hist.at[k, steps], steps % 2)
    mid_wait_send()
    mid_product(0)
    h2_load.wait()
    h0_copy.wait()
    moved_rows = wh2.at[1, pl.ds(pl.multiple_of(data * half, 16), half)]
    came_rows = wh2.at[1, pl.ds(pl.multiple_of((1 - data) * half, 16), half)]
    pltpu.make_async_remote_copy(
        src_ref=moved_rows, dst_ref=moved_rows, send_sem=move_send, recv_sem=move_recv.at[0],
        device_id={'row': across}, device_id_type=MESH).wait_send()
    pltpu.make_async_remote_copy(
        src_ref=moved_rows, dst_ref=came_rows, send_sem=relay_send, recv_sem=relay_recv,
        device_id={'data': 1 - data}, device_id_type=MESH).wait()

    def layer_two(n, carry):
        slot = n % 2

        @pl.when(n > 0)
        def _():
            h2_wait_recv(slot)
        a = [joined(h2b.at[slot, p]) for p in range(2)]
        for idx, part in ((0, 1 - core), (3, core)):
            cols = pl.ds(pl.multiple_of(part * width, LANES), width)
            zp[0, idx] = dot(a[0], wh2[0, :, cols]) + dot(a[1], wh2[1, :, cols])
            if idx == 0:
                mate_copy(0, slot, 0).start()
        mate_copy(0, slot, 0).wait_recv()
        mid_slot = n % 3
        mid_mate_copy(mid_slot, 1).wait_recv()
        mid_across_copy(mid_slot).wait_recv()
        h = gates(2, b2_ref, 0, (zp.at[0, 3], p1r.at[0, slot, 0], zm.at[slot],
                                 m1r.at[mid_slot, 1], myr.at[mid_slot]))
        mate_copy(0, slot, 0).wait_send()

        @pl.when(n > 0)
        def _():
            h2_wait_send(slot)
        hsend[2] = h
        out_ref[n] = h

        @pl.when(n < steps - 1)
        def _():
            h2_start(1 - slot)

        @pl.when(n < steps - 2)
        def _():
            mid_wait_send()
            mid_product(n + 2)
        return carry

    lax.fori_loop(0, steps, layer_two, 0)
    mid_wait_send()
    for k in range(3):
        c_out[k] = moved(c_ref[k], sel[...])


def solution(mesh):
    n_data = mesh.shape['data']
    n_row = mesh.shape['row']
    n_col = mesh.shape['col']
    spec_seq = P(None, 'data', 'row')
    spec_weight = P(None, 'row', 'col')
    spec_out = P(None, 'data', ('col', 'row'))

    def local(x_rows, w_x1, w_h1, b_1, w_x2, w_h2, b_2, h_zero, c_zero):
        steps, batch, d_row = x_rows.shape
        unit_n = d_row // n_col
        width = 4 * unit_n
        vmem = pl.BlockSpec(memory_space=pltpu.VMEM)
        hbm = pl.BlockSpec(memory_space=pl.ANY)
        dma = pltpu.SemaphoreType.DMA
        return pl.pallas_call(
            functools.partial(lstm_kernel, steps, n_data, n_row, n_col),
            out_shape=(jax.ShapeDtypeStruct((steps, batch, unit_n), BF16),
                       jax.ShapeDtypeStruct((3, batch, unit_n), F32)),
            in_specs=[vmem, hbm, hbm, hbm, hbm, vmem, vmem, vmem, vmem],
            out_specs=(vmem, vmem),
            scratch_shapes=[
                pltpu.VMEM((2, 4, d_row, width), BF16),
                pltpu.VMEM((2, 4, d_row, width), BF16),
                pltpu.VMEM((2, d_row, 2 * width), BF16),
                pltpu.VMEM((2, steps + 1, n_row, batch, unit_n), BF16),
                pltpu.VMEM((2, 2, n_row, batch, unit_n), BF16),
                pltpu.VMEM((2, 4, batch, width), F32),
                pltpu.VMEM((2, 2, 2, batch, width), F32),
                pltpu.VMEM((2, 2, batch, width), F32),
                pltpu.VMEM((2, batch, width), F32),
                pltpu.VMEM((3, 2, batch, width), F32),
                pltpu.VMEM((3, batch, width), F32),
                pltpu.VMEM((3, batch, unit_n), BF16),
                pltpu.VMEM((width, unit_n), BF16),
                pltpu.VMEM((unit_n, width), BF16),
                pltpu.VMEM((3, batch, unit_n), F32),
                pltpu.VMEM((3, batch, width), F32),
                dma((2,)),
                dma((7, 4)), dma((2, 2)), dma((2, 2, 2)), dma((2,)), dma((2, 2)),
                dma((2,)), dma((3, 2)), dma, dma((3,)),
                dma((2, n_col)), dma((2, 2, n_row)), dma((n_col, 2)), dma((2, 2, n_row)),
                dma((2,)), dma, dma((8,)), dma, dma,
            ],
            compiler_params=pltpu.CompilerParams(
                collective_id=0, has_side_effects=True, vmem_limit_bytes=60 * 1024 * 1024),
        )(x_rows, w_x1, w_h1, w_x2, w_h2, b_1, b_2[None], h_zero, c_zero)

    return jax.shard_map(local, mesh=mesh,
                         in_specs=(spec_seq, spec_weight, spec_weight, P(None, 'col'), spec_weight,
                                   P('row', 'col'), P('col'), spec_seq, spec_seq),
                         out_specs=(spec_out, spec_out), check_vma=False)
```

```python
import functools

import jax
import jax.numpy as jnp
from jax import lax
from jax.experimental import pallas as pl
from jax.experimental.pallas import tpu as pltpu
from jax.sharding import PartitionSpec as P

MESH = pl.DeviceIdType.MESH
F32 = jnp.float32
BF16 = jnp.bfloat16
LANES = 128
SPLIT = 2


def lstm_kernel(steps, n_data, n_row, n_col,
                x_ref, wx1_hbm, wh1_hbm, wx2_hbm, wh2_hbm, b1_ref, b2_ref, h0_ref, c0_ref,
                out_ref, c_out,
                wx, wh, wh2, hist, h2b, zp, p1r, yr, zm, m1r, myr, hsend, sel, spread, c_own, c_ref,
                c_sem, w_sem, p1_send, p1_recv, y_send, y_recv, m1_send, m1_recv, my_send, my_recv,
                h_send, h_recv, h2_send, h2_recv, h0_sem, move_send, move_recv, relay_send, relay_recv):
    data = lax.axis_index('data')
    row = lax.axis_index('row')
    col = lax.axis_index('col')
    batch, d_row = x_ref.shape[1], x_ref.shape[2]
    unit_n = d_row // n_col
    width = 4 * unit_n
    part_n = width // SPLIT
    core = row % 2
    mate = row + 1 - 2 * core
    across = (row + 2) % 4
    order = (3 - row, across, mate, row)

    def weight_copy(src, dst, idx, sem):
        cols = pl.ds(pl.multiple_of(order[idx] * width, LANES), width)
        return pltpu.make_async_copy(src.at[:, cols], dst.at[idx], w_sem.at[sem, idx])

    loads = {'x0': (wx1_hbm.at[0], wx.at[0], 0), 'h0': (wh1_hbm.at[0], wh.at[0], 1),
             'x1': (wx1_hbm.at[1], wx.at[1], 2), 'h1': (wh1_hbm.at[1], wh.at[1], 3),
             'm0': (wx2_hbm.at[0], wx.at[0], 4), 'm1': (wx2_hbm.at[1], wx.at[1], 5)}

    def load_start(name):
        for idx in range(4):
            src, dst, sem = loads[name]
            weight_copy(src, dst, idx, sem).start()

    def load_wait(name):
        for idx in range(4):
            src, dst, sem = loads[name]
            weight_copy(src, dst, idx, sem).wait()

    for name in ('x0', 'h0', 'x1', 'h1'):
        load_start(name)

    half = d_row // 2
    piece = half // (2 * steps)
    own_cols = pl.ds(pl.multiple_of(row // 2 * (2 * width), LANES), 2 * width)
    far_cols = pl.ds(pl.multiple_of((1 - row // 2) * (2 * width), LANES), 2 * width)
    h2_load = pltpu.make_async_copy(wh2_hbm.at[:, own_cols], wh2.at[0], w_sem.at[6, 0])
    h2_load.start()

    def piece_rows(part, p):
        return pl.ds(pl.multiple_of(part * half + p * piece, 16), piece)

    def move_copy(p):
        rows = piece_rows(data, p)
        return pltpu.make_async_remote_copy(
            src_ref=wh2_hbm.at[rows, far_cols], dst_ref=wh2.at[1, rows],
            send_sem=move_send, recv_sem=move_recv.at[p % 8],
            device_id={'row': across}, device_id_type=MESH)

    def relay_copy(p):
        rows = piece_rows(data, p)
        return pltpu.make_async_remote_copy(
            src_ref=wh2.at[1, rows], dst_ref=wh2.at[1, rows],
            send_sem=relay_send, recv_sem=relay_recv,
            device_id={'data': 1 - data}, device_id_type=MESH)

    def forward(p):
        move_copy(p).wait_recv()
        relay_copy(p).start()

    barrier = pltpu.get_barrier_semaphore()
    for dc in range(n_col):
        for dr in range(n_row):
            if dc or dr:
                pl.semaphore_signal(barrier, inc=1, device_id_type=MESH,
                                    device_id={'col': (col + dc) % n_col, 'row': (row + dr) % n_row})
    pl.semaphore_signal(barrier, inc=1, device_id_type=MESH, device_id={'data': 1 - data})

    rr = lax.broadcasted_iota(jnp.int32, (width, unit_n), 0)
    cc = lax.broadcasted_iota(jnp.int32, (width, unit_n), 1)
    sel[...] = jnp.where(rr == 4 * cc, 1.0, 0.0).astype(BF16)
    for k in range(2):
        for j in range(n_row):
            hist[k, 0, j] = h0_ref[k, :, j * unit_n:(j + 1) * unit_n].astype(BF16)
    for j in range(n_row):
        h2b[0, 0, j] = h0_ref[2, :, j * unit_n:(j + 1) * unit_n].astype(BF16)
    rr = lax.broadcasted_iota(jnp.int32, (unit_n, width), 0)
    cc = lax.broadcasted_iota(jnp.int32, (unit_n, width), 1)
    spread[...] = jnp.where(rr == cc // 4, 1.0, 0.0).astype(BF16)

    own_stays = row == col
    c_part = pl.ds(pl.multiple_of(col * unit_n, LANES), unit_n)
    c_copy = pltpu.make_async_remote_copy(
        src_ref=c0_ref.at[:, :, c_part], dst_ref=c_own, send_sem=c_sem.at[0], recv_sem=c_sem.at[1],
        device_id={'col': row, 'row': col}, device_id_type=MESH)
    pl.semaphore_wait(barrier, n_col * n_row)

    @pl.when(jnp.logical_not(own_stays))
    def _():
        c_copy.start()

    @pl.when(own_stays)
    def _():
        c_own[...] = c0_ref[:, :, c_part]

    h0_copy = pltpu.make_async_remote_copy(
        src_ref=h2b.at[0, 0], dst_ref=h2b.at[0, 1], send_sem=h0_sem.at[0], recv_sem=h0_sem.at[1],
        device_id={'row': across}, device_id_type=MESH)
    h0_copy.start()

    def dot(a, w):
        return jnp.dot(a, w, preferred_element_type=F32)

    def lanes_of(s):
        return slice(s * part_n, (s + 1) * part_n)

    def moved(a, m):
        a = a * 0.5
        top = a.astype(BF16)
        rest = a - top.astype(F32)
        mid = rest.astype(BF16)
        low = (rest - mid.astype(F32)).astype(BF16)
        parts = dot(jnp.concatenate([top, mid, low], axis=0), m)
        return ((parts[:batch] + parts[batch:2 * batch]) + parts[2 * batch:]) * 2.0

    def joined(blocks):
        return jnp.concatenate([blocks[j] for j in range(n_row)], axis=1)

    def input_product(k, t):
        a = x_ref[t]
        for idx in range(4):
            for s in range(SPLIT):
                zp[k, idx, s] = dot(a, wx[k, idx, :, lanes_of(s)])

    load_wait('x0')
    input_product(0, 0)
    load_wait('x1')
    input_product(1, steps - 1)
    load_wait('h0')
    load_wait('h1')

    @pl.when(jnp.logical_not(own_stays))
    def _():
        c_copy.wait()
    for k in range(3):
        c_ref[k] = moved(c_own[k], spread[...])

    def mate_copy(k, slot, part, s):
        return pltpu.make_async_remote_copy(
            src_ref=zp.at[k, 2 * part, s], dst_ref=p1r.at[k, slot, part, s],
            send_sem=p1_send.at[k, part, s], recv_sem=p1_recv.at[k, slot, part, s],
            device_id={'row': mate}, device_id_type=MESH)

    def across_copy(k, slot, s):
        return pltpu.make_async_remote_copy(
            src_ref=zp.at[k, 1, s], dst_ref=yr.at[k, slot, s],
            send_sem=y_send.at[k, s], recv_sem=y_recv.at[k, slot, s],
            device_id={'row': across}, device_id_type=MESH)

    def far(i):
        return (n_col - 1 - i) + (2 * i - (n_col - 1)) * (col // (n_col // 2))

    def h_copy(k, dst, slot, i):
        return pltpu.make_async_remote_copy(
            src_ref=hsend.at[k], dst_ref=dst.at[row],
            send_sem=h_send.at[k, i], recv_sem=h_recv.at[k, slot, row],
            device_id={'col': far(i), 'row': col}, device_id_type=MESH)

    def h_start(k, dst, slot):
        for i in range(n_col):
            pl.when(jnp.logical_not(own_stays & (far(i) == col)))(lambda i=i: h_copy(k, dst, slot, i).start())

        @pl.when(own_stays)
        def _():
            dst[row] = hsend[k]

    def h_wait_send(k, dst, slot):
        for i in range(n_col):
            pl.when(jnp.logical_not(own_stays & (far(i) == col)))(lambda i=i: h_copy(k, dst, slot, i).wait_send())

    def h_wait_recv(k, dst, slot):
        for j in range(n_row):
            def wait(j=j):
                pltpu.make_async_remote_copy(
                    src_ref=hsend.at[k], dst_ref=dst.at[j],
                    send_sem=h_send.at[k, 0], recv_sem=h_recv.at[k, slot, j],
                    device_id={'col': col, 'row': row}, device_id_type=MESH).wait_recv()
            pl.when(jnp.logical_not(own_stays & (row == j)))(wait)

    def head(k, slot, blocks, w_rec):
        a = joined(blocks)
        todo = []

        def finish(idx, s, z):
            zp[k, idx, s] = zp[k, idx, s] + z
            if idx % 2 == 0:
                mate_copy(k, slot, idx // 2, s).start()

        for idx in range(4):
            for s in range(SPLIT):
                todo.append((idx, s, dot(a, w_rec[idx, :, lanes_of(s)])))
                if len(todo) > 1:
                    finish(*todo.pop(0))
            if idx == 2:
                finish(*todo.pop(0))
                middle(k, slot)
        finish(*todo.pop(0))

    def middle(k, slot):
        for s in range(SPLIT):
            mate_copy(k, slot, 0, s).wait_recv()
            zp[k, 1, s] = zp[k, 1, s] + p1r[k, slot, 0, s]
            across_copy(k, slot, s).start()

    def gates(cell, bias_ref, bias_row, addends):
        gate = lax.broadcasted_iota(jnp.int32, (batch, LANES), 1) % 4
        scale = jnp.where(gate == 2, 1.0, 0.5)
        shift = jnp.where(gate == 2, 0.0, 0.5)
        pieces = []
        for p in range(width // LANES):
            lanes = slice(p * LANES, (p + 1) * LANES)
            z = bias_ref[bias_row:bias_row + 1, pl.ds(pl.multiple_of(row * width, LANES) + p * LANES, LANES)]
            for a in addends:
                z = z + a[p * LANES // part_n, :, pl.ds(p * LANES % part_n, LANES)]
            act = jnp.tanh(z * scale) * scale + shift
            f = pltpu.roll(act, LANES - 1, 1)
            g = pltpu.roll(act, LANES - 2, 1)
            o = pltpu.roll(act, LANES - 3, 1)
            c_new = f * c_ref[cell, :, lanes] + act * g
            c_ref[cell, :, lanes] = c_new
            pieces.append((o * jnp.tanh(c_new)).astype(BF16))
        return dot(jnp.concatenate(pieces, axis=1), sel[...]).astype(BF16)

    def gates_one(k, slot):
        for s in range(SPLIT):
            mate_copy(k, slot, 1, s).wait_recv()
            across_copy(k, slot, s).wait_recv()
        h = gates(k, b1_ref, k, (zp.at[k, 3], p1r.at[k, slot, 1], yr.at[k, slot]))
        for s in range(SPLIT):
            for part in range(2):
                mate_copy(k, slot, part, s).wait_send()
            across_copy(k, slot, s).wait_send()
        return h

    def layer_one(n, carry):
        slot = n % 2
        for k in range(2):
            @pl.when(n > 0)
            def _(k=k):
                h_wait_recv(k, hist.at[k, n], slot)
            head(k, slot, hist.at[k, n], wh.at[k])
        for k in range(2):
            h = gates_one(k, slot)

            @pl.when(n > 0)
            def _(k=k):
                h_wait_send(k, hist.at[k, n], slot)
            hsend[k] = h
            h_start(k, hist.at[k, n + 1], (n + 1) % 2)

            @pl.when(n > 0)
            def _(k=k):
                forward(2 * n - 2 + k)

            if k == 1:
                move_copy(2 * n).start()
                move_copy(2 * n + 1).start()

            @pl.when(n < steps - 1)
            def _(k=k):
                input_product(k, n + 1 if k == 0 else steps - 2 - n)

            @pl.when(n == steps - 1)
            def _(k=k):
                load_start('m0' if k == 0 else 'm1')
        return carry

    lax.fori_loop(0, steps, layer_one, 0)

    def mid_mate_copy(slot, part):
        return pltpu.make_async_remote_copy(
            src_ref=zp.at[1, 2 * part], dst_ref=m1r.at[slot, part],
            send_sem=m1_send.at[part], recv_sem=m1_recv.at[slot, part],
            device_id={'row': mate}, device_id_type=MESH)

    def mid_across_copy(slot):
        return pltpu.make_async_remote_copy(
            src_ref=zp.at[1, 1], dst_ref=myr.at[slot],
            send_sem=my_send, recv_sem=my_recv.at[slot],
            device_id={'row': across}, device_id_type=MESH)

    def mid_wait_send():
        for part in range(2):
            mid_mate_copy(0, part).wait_send()
        mid_across_copy(0).wait_send()

    def mid_product(t):
        slot = t % 3
        a = joined(hist.at[0, t + 1])
        b = joined(hist.at[1, steps - t])
        for idx in range(4):
            for s in range(SPLIT):
                z = dot(a, wx[0, idx, :, lanes_of(s)]) + dot(b, wx[1, idx, :, lanes_of(s)])
                if idx < 3:
                    zp[1, idx, s] = z
                else:
                    zm[t % 2, s] = z
            if idx % 2 == 0:
                mid_mate_copy(slot, idx // 2).start()
        mid_mate_copy(slot, 0).wait_recv()
        zp[1, 1] = zp[1, 1] + m1r[slot, 0]
        mid_across_copy(slot).start()

    def h2_copy(slot, i, p):
        return pltpu.make_async_remote_copy(
            src_ref=hsend.at[2], dst_ref=h2b.at[slot, p, row],
            send_sem=h2_send.at[i, p], recv_sem=h2_recv.at[slot, p, row],
            device_id={'col': far(i), 'row': (col + 2 * p) % n_row}, device_id_type=MESH)

    h2_stays = [row == (col + 2 * p) % n_row for p in range(2)]

    def h2_start(slot):
        for i in range(n_col):
            for p in range(2):
                pl.when(jnp.logical_not(h2_stays[p] & (far(i) == col)))(lambda i=i, p=p: h2_copy(slot, i, p).start())
        for p in range(2):
            @pl.when(h2_stays[p])
            def _(p=p):
                h2b[slot, p, row] = hsend[2]

    def h2_wait_send(slot):
        for i in range(n_col):
            for p in range(2):
                pl.when(jnp.logical_not(h2_stays[p] & (far(i) == col)))(
                    lambda i=i, p=p: h2_copy(slot, i, p).wait_send())

    def h2_wait_recv(slot):
        for p in range(2):
            for j in range(n_row):
                def wait(p=p, j=j):
                    pltpu.make_async_remote_copy(
                        src_ref=hsend.at[2], dst_ref=h2b.at[slot, p, j],
                        send_sem=h2_send.at[0, 0], recv_sem=h2_recv.at[slot, p, j],
                        device_id={'col': col, 'row': row}, device_id_type=MESH).wait_recv()
                pl.when(jnp.logical_not(h2_stays[p] & (row == j)))(wait)

    for k in range(2):
        forward(2 * steps - 2 + k)
    for k in range(2):
        h_wait_send(k, hist.at[k, steps], steps % 2)
    for name in ('m0', 'm1'):
        load_wait(name)
    mid_product(1)
    for k in range(2):
        h_wait_recv(k, hist.at[k, steps], steps % 2)
    mid_wait_send()
    mid_product(0)
    h2_load.wait()
    h0_copy.wait()
    moved_rows = wh2.at[1, pl.ds(pl.multiple_of(data * half, 16), half)]
    came_rows = wh2.at[1, pl.ds(pl.multiple_of((1 - data) * half, 16), half)]
    pltpu.make_async_remote_copy(
        src_ref=moved_rows, dst_ref=moved_rows, send_sem=move_send, recv_sem=move_recv.at[0],
        device_id={'row': across}, device_id_type=MESH).wait_send()
    pltpu.make_async_remote_copy(
        src_ref=moved_rows, dst_ref=came_rows, send_sem=relay_send, recv_sem=relay_recv,
        device_id={'data': 1 - data}, device_id_type=MESH).wait()

    def layer_two(n, carry):
        slot = n % 2

        @pl.when(n > 0)
        def _():
            h2_wait_recv(slot)
        a = [joined(h2b.at[slot, p]) for p in range(2)]
        todo = []

        def finish(idx, s, z):
            zp[0, idx, s] = z
            if idx == 0:
                mate_copy(0, slot, 0, s).start()

        for idx, part in ((0, 1 - core), (3, core)):
            for s in range(SPLIT):
                cols = pl.ds(pl.multiple_of(part * width + s * part_n, LANES), part_n)
                todo.append((idx, s, dot(a[0], wh2[0, :, cols]) + dot(a[1], wh2[1, :, cols])))
                if len(todo) > 1:
                    finish(*todo.pop(0))
        finish(*todo.pop(0))
        for s in range(SPLIT):
            mate_copy(0, slot, 0, s).wait_recv()
        mid_slot = n % 3
        mid_mate_copy(mid_slot, 1).wait_recv()
        mid_across_copy(mid_slot).wait_recv()
        h = gates(2, b2_ref, 0, (zp.at[0, 3], p1r.at[0, slot, 0], zm.at[slot],
                                 m1r.at[mid_slot, 1], myr.at[mid_slot]))
        for s in range(SPLIT):
            mate_copy(0, slot, 0, s).wait_send()

        @pl.when(n > 0)
        def _():
            h2_wait_send(slot)
        hsend[2] = h
        out_ref[n] = h

        @pl.when(n < steps - 1)
        def _():
            h2_start(1 - slot)

        @pl.when(n < steps - 2)
        def _():
            mid_wait_send()
            mid_product(n + 2)
        return carry

    lax.fori_loop(0, steps, layer_two, 0)
    mid_wait_send()
    for k in range(3):
        c_out[k] = moved(c_ref[k], sel[...])


def solution(mesh):
    n_data = mesh.shape['data']
    n_row = mesh.shape['row']
    n_col = mesh.shape['col']
    spec_seq = P(None, 'data', 'row')
    spec_weight = P(None, 'row', 'col')
    spec_out = P(None, 'data', ('col', 'row'))

    def local(x_rows, w_x1, w_h1, b_1, w_x2, w_h2, b_2, h_zero, c_zero):
        steps, batch, d_row = x_rows.shape
        unit_n = d_row // n_col
        width = 4 * unit_n
        vmem = pl.BlockSpec(memory_space=pltpu.VMEM)
        hbm = pl.BlockSpec(memory_space=pl.ANY)
        dma = pltpu.SemaphoreType.DMA
        return pl.pallas_call(
            functools.partial(lstm_kernel, steps, n_data, n_row, n_col),
            out_shape=(jax.ShapeDtypeStruct((steps, batch, unit_n), BF16),
                       jax.ShapeDtypeStruct((3, batch, unit_n), F32)),
            in_specs=[vmem, hbm, hbm, hbm, hbm, vmem, vmem, vmem, vmem],
            out_specs=(vmem, vmem),
            scratch_shapes=[
                pltpu.VMEM((2, 4, d_row, width), BF16),
                pltpu.VMEM((2, 4, d_row, width), BF16),
                pltpu.VMEM((2, d_row, 2 * width), BF16),
                pltpu.VMEM((2, steps + 1, n_row, batch, unit_n), BF16),
                pltpu.VMEM((2, 2, n_row, batch, unit_n), BF16),
                pltpu.VMEM((2, 4, SPLIT, batch, width // SPLIT), F32),
                pltpu.VMEM((2, 2, 2, SPLIT, batch, width // SPLIT), F32),
                pltpu.VMEM((2, 2, SPLIT, batch, width // SPLIT), F32),
                pltpu.VMEM((2, SPLIT, batch, width // SPLIT), F32),
                pltpu.VMEM((3, 2, SPLIT, batch, width // SPLIT), F32),
                pltpu.VMEM((3, SPLIT, batch, width // SPLIT), F32),
                pltpu.VMEM((3, batch, unit_n), BF16),
                pltpu.VMEM((width, unit_n), BF16),
                pltpu.VMEM((unit_n, width), BF16),
                pltpu.VMEM((3, batch, unit_n), F32),
                pltpu.VMEM((3, batch, width), F32),
                dma((2,)),
                dma((7, 4)), dma((2, 2, SPLIT)), dma((2, 2, 2, SPLIT)), dma((2, SPLIT)), dma((2, 2, SPLIT)),
                dma((2,)), dma((3, 2)), dma, dma((3,)),
                dma((2, n_col)), dma((2, 2, n_row)), dma((n_col, 2)), dma((2, 2, n_row)),
                dma((2,)), dma, dma((8,)), dma, dma,
            ],
            compiler_params=pltpu.CompilerParams(
                collective_id=0, has_side_effects=True, vmem_limit_bytes=60 * 1024 * 1024),
        )(x_rows, w_x1, w_h1, w_x2, w_h2, b_1, b_2[None], h_zero, c_zero)

    return jax.shard_map(local, mesh=mesh,
                         in_specs=(spec_seq, spec_weight, spec_weight, P(None, 'col'), spec_weight,
                                   P('row', 'col'), P('col'), spec_seq, spec_seq),
                         out_specs=(spec_out, spec_out), check_vma=False)
```

```python
import functools

import jax
import jax.numpy as jnp
from jax import lax
from jax.experimental import pallas as pl
from jax.experimental.pallas import tpu as pltpu
from jax.sharding import PartitionSpec as P

MESH = pl.DeviceIdType.MESH
F32 = jnp.float32
BF16 = jnp.bfloat16
LANES = 128
SPLIT = 2


def lstm_kernel(steps, n_data, n_row, n_col,
                x_ref, wx1_hbm, wh1_hbm, wx2_hbm, wh2_hbm, b1_ref, b2_ref, h0_ref, c0_ref,
                out_ref, c_out,
                wx, wh, wh2, hist, h2b, zp, p1r, yr, zm, m1r, myr, hsend, sel, spread, c_own, c_ref,
                c_sem, w_sem, p1_send, p1_recv, y_send, y_recv, m1_send, m1_recv, my_send, my_recv,
                h_send, h_recv, h2_send, h2_recv, h0_sem, move_send, move_recv, relay_send, relay_recv):
    data = lax.axis_index('data')
    row = lax.axis_index('row')
    col = lax.axis_index('col')
    batch, d_row = x_ref.shape[1], x_ref.shape[2]
    unit_n = d_row // n_col
    width = 4 * unit_n
    part_n = width // SPLIT
    core = row % 2
    mate = row + 1 - 2 * core
    across = (row + 2) % 4
    order = (3 - row, across, mate, row)

    def weight_copy(src, dst, idx, sem):
        cols = pl.ds(pl.multiple_of(order[idx] * width, LANES), width)
        return pltpu.make_async_copy(src.at[:, cols], dst.at[idx], w_sem.at[sem, idx])

    loads = {'x0': (wx1_hbm.at[0], wx.at[0], 0), 'h0': (wh1_hbm.at[0], wh.at[0], 1),
             'x1': (wx1_hbm.at[1], wx.at[1], 2), 'h1': (wh1_hbm.at[1], wh.at[1], 3),
             'm0': (wx2_hbm.at[0], wx.at[0], 4), 'm1': (wx2_hbm.at[1], wx.at[1], 5)}

    def load_start(name):
        for idx in range(4):
            src, dst, sem = loads[name]
            weight_copy(src, dst, idx, sem).start()

    def load_wait(name):
        for idx in range(4):
            src, dst, sem = loads[name]
            weight_copy(src, dst, idx, sem).wait()

    for name in ('x0', 'h0', 'x1', 'h1'):
        load_start(name)

    half = d_row // 2
    piece = half // (2 * steps)
    own_cols = pl.ds(pl.multiple_of(row // 2 * (2 * width), LANES), 2 * width)
    far_cols = pl.ds(pl.multiple_of((1 - row // 2) * (2 * width), LANES), 2 * width)
    h2_load = pltpu.make_async_copy(wh2_hbm.at[:, own_cols], wh2.at[0], w_sem.at[6, 0])
    h2_load.start()

    def piece_rows(part, p):
        return pl.ds(pl.multiple_of(part * half + p * piece, 16), piece)

    def move_copy(p):
        rows = piece_rows(data, p)
        return pltpu.make_async_remote_copy(
            src_ref=wh2_hbm.at[rows, far_cols], dst_ref=wh2.at[1, rows],
            send_sem=move_send, recv_sem=move_recv.at[p % 8],
            device_id={'row': across}, device_id_type=MESH)

    def relay_copy(p):
        rows = piece_rows(data, p)
        return pltpu.make_async_remote_copy(
            src_ref=wh2.at[1, rows], dst_ref=wh2.at[1, rows],
            send_sem=relay_send, recv_sem=relay_recv,
            device_id={'data': 1 - data}, device_id_type=MESH)

    def forward(p):
        move_copy(p).wait_recv()
        relay_copy(p).start()

    barrier = pltpu.get_barrier_semaphore()
    for dc in range(n_col):
        for dr in range(n_row):
            if dc or dr:
                pl.semaphore_signal(barrier, inc=1, device_id_type=MESH,
                                    device_id={'col': (col + dc) % n_col, 'row': (row + dr) % n_row})
    pl.semaphore_signal(barrier, inc=1, device_id_type=MESH, device_id={'data': 1 - data})

    rr = lax.broadcasted_iota(jnp.int32, (width, unit_n), 0)
    cc = lax.broadcasted_iota(jnp.int32, (width, unit_n), 1)
    sel[...] = jnp.where(rr == 4 * cc, 1.0, 0.0).astype(BF16)
    for k in range(2):
        for j in range(n_row):
            hist[k, 0, j] = h0_ref[k, :, j * unit_n:(j + 1) * unit_n].astype(BF16)
    for j in range(n_row):
        h2b[0, 0, j] = h0_ref[2, :, j * unit_n:(j + 1) * unit_n].astype(BF16)
    rr = lax.broadcasted_iota(jnp.int32, (unit_n, width), 0)
    cc = lax.broadcasted_iota(jnp.int32, (unit_n, width), 1)
    spread[...] = jnp.where(rr == cc // 4, 1.0, 0.0).astype(BF16)

    own_stays = row == col
    c_part = pl.ds(pl.multiple_of(col * unit_n, LANES), unit_n)
    c_copy = pltpu.make_async_remote_copy(
        src_ref=c0_ref.at[:, :, c_part], dst_ref=c_own, send_sem=c_sem.at[0], recv_sem=c_sem.at[1],
        device_id={'col': row, 'row': col}, device_id_type=MESH)
    pl.semaphore_wait(barrier, n_col * n_row)

    @pl.when(jnp.logical_not(own_stays))
    def _():
        c_copy.start()

    @pl.when(own_stays)
    def _():
        c_own[...] = c0_ref[:, :, c_part]

    h0_copy = pltpu.make_async_remote_copy(
        src_ref=h2b.at[0, 0], dst_ref=h2b.at[0, 1], send_sem=h0_sem.at[0], recv_sem=h0_sem.at[1],
        device_id={'row': across}, device_id_type=MESH)
    h0_copy.start()

    def dot(a, w):
        return jnp.dot(a, w, preferred_element_type=F32)

    def lanes_of(s):
        return slice(s * part_n, (s + 1) * part_n)

    def moved(a, m):
        a = a * 0.5
        top = a.astype(BF16)
        rest = a - top.astype(F32)
        mid = rest.astype(BF16)
        low = (rest - mid.astype(F32)).astype(BF16)
        parts = dot(jnp.concatenate([top, mid, low], axis=0), m)
        return ((parts[:batch] + parts[batch:2 * batch]) + parts[2 * batch:]) * 2.0

    def joined(blocks):
        return jnp.concatenate([blocks[j] for j in range(n_row)], axis=1)

    def input_product(k, t):
        a = x_ref[t]
        for idx in range(4):
            for s in range(SPLIT):
                zp[k, idx, s] = dot(a, wx[k, idx, :, lanes_of(s)])

    load_wait('x0')
    input_product(0, 0)
    load_wait('h0')

    @pl.when(jnp.logical_not(own_stays))
    def _():
        c_copy.wait()
    for k in range(3):
        c_ref[k] = moved(c_own[k], spread[...])

    def mate_copy(k, slot, part, s):
        return pltpu.make_async_remote_copy(
            src_ref=zp.at[k, 2 * part, s], dst_ref=p1r.at[k, slot, part, s],
            send_sem=p1_send.at[k, part, s], recv_sem=p1_recv.at[k, slot, part, s],
            device_id={'row': mate}, device_id_type=MESH)

    def across_copy(k, slot, s):
        return pltpu.make_async_remote_copy(
            src_ref=zp.at[k, 1, s], dst_ref=yr.at[k, slot, s],
            send_sem=y_send.at[k, s], recv_sem=y_recv.at[k, slot, s],
            device_id={'row': across}, device_id_type=MESH)

    def far(i):
        return (n_col - 1 - i) + (2 * i - (n_col - 1)) * (col // (n_col // 2))

    def h_copy(k, dst, slot, i):
        return pltpu.make_async_remote_copy(
            src_ref=hsend.at[k], dst_ref=dst.at[row],
            send_sem=h_send.at[k, i], recv_sem=h_recv.at[k, slot, row],
            device_id={'col': far(i), 'row': col}, device_id_type=MESH)

    def h_start(k, dst, slot):
        for i in range(n_col):
            pl.when(jnp.logical_not(own_stays & (far(i) == col)))(lambda i=i: h_copy(k, dst, slot, i).start())

        @pl.when(own_stays)
        def _():
            dst[row] = hsend[k]

    def h_wait_send(k, dst, slot):
        for i in range(n_col):
            pl.when(jnp.logical_not(own_stays & (far(i) == col)))(lambda i=i: h_copy(k, dst, slot, i).wait_send())

    def h_wait_recv(k, dst, slot):
        for j in range(n_row):
            def wait(j=j):
                pltpu.make_async_remote_copy(
                    src_ref=hsend.at[k], dst_ref=dst.at[j],
                    send_sem=h_send.at[k, 0], recv_sem=h_recv.at[k, slot, j],
                    device_id={'col': col, 'row': row}, device_id_type=MESH).wait_recv()
            pl.when(jnp.logical_not(own_stays & (row == j)))(wait)

    def head(k, slot, blocks, w_rec):
        a = joined(blocks)
        todo = []

        def finish(idx, s, z):
            zp[k, idx, s] = zp[k, idx, s] + z
            if idx % 2 == 0:
                mate_copy(k, slot, idx // 2, s).start()

        for idx in range(4):
            for s in range(SPLIT):
                todo.append((idx, s, dot(a, w_rec[idx, :, lanes_of(s)])))
                if len(todo) > 1:
                    finish(*todo.pop(0))
            if idx == 2:
                finish(*todo.pop(0))
                pl.when(core == 0)(lambda: middle(k, slot))
        finish(*todo.pop(0))
        if k:
            pl.when(core != 0)(lambda: middle(k, slot))

    def middle(k, slot):
        for s in range(SPLIT):
            mate_copy(k, slot, 0, s).wait_recv()
            zp[k, 1, s] = zp[k, 1, s] + p1r[k, slot, 0, s]
            across_copy(k, slot, s).start()

    def gates(cell, bias_ref, bias_row, addends):
        gate = lax.broadcasted_iota(jnp.int32, (batch, LANES), 1) % 4
        scale = jnp.where(gate == 2, 1.0, 0.5)
        shift = jnp.where(gate == 2, 0.0, 0.5)
        pieces = []
        for p in range(width // LANES):
            lanes = slice(p * LANES, (p + 1) * LANES)
            z = bias_ref[bias_row:bias_row + 1, pl.ds(pl.multiple_of(row * width, LANES) + p * LANES, LANES)]
            for a in addends:
                z = z + a[p * LANES // part_n, :, pl.ds(p * LANES % part_n, LANES)]
            act = jnp.tanh(z * scale) * scale + shift
            f = pltpu.roll(act, LANES - 1, 1)
            g = pltpu.roll(act, LANES - 2, 1)
            o = pltpu.roll(act, LANES - 3, 1)
            c_new = f * c_ref[cell, :, lanes] + act * g
            c_ref[cell, :, lanes] = c_new
            pieces.append((o * jnp.tanh(c_new)).astype(BF16))
        return dot(jnp.concatenate(pieces, axis=1), sel[...]).astype(BF16)

    def gates_one(k, slot):
        for s in range(SPLIT):
            mate_copy(k, slot, 1, s).wait_recv()
            across_copy(k, slot, s).wait_recv()
        h = gates(k, b1_ref, k, (zp.at[k, 3], p1r.at[k, slot, 1], yr.at[k, slot]))
        for s in range(SPLIT):
            for part in range(2):
                mate_copy(k, slot, part, s).wait_send()
            across_copy(k, slot, s).wait_send()
        return h

    def layer_one(n, carry):
        slot = n % 2
        for k in range(2):
            if k == 1:
                pl.when(n == 0)(lambda: load_wait('x1'))
                input_product(1, steps - 1 - n)
                pl.when(core != 0)(lambda: middle(0, slot))
                pl.when(n == 0)(lambda: load_wait('h1'))
                pl.when(n == steps - 1)(lambda: load_start('m1'))

            @pl.when(n > 0)
            def _(k=k):
                h_wait_recv(k, hist.at[k, n], slot)
            head(k, slot, hist.at[k, n], wh.at[k])
        for k in range(2):
            h = gates_one(k, slot)

            @pl.when(n > 0)
            def _(k=k):
                h_wait_send(k, hist.at[k, n], slot)
            hsend[k] = h
            h_start(k, hist.at[k, n + 1], (n + 1) % 2)

            @pl.when(n > 0)
            def _(k=k):
                forward(2 * n - 2 + k)

            if k == 0:
                move_copy(2 * n).start()
                move_copy(2 * n + 1).start()

            if k == 0:
                @pl.when(n < steps - 1)
                def _():
                    input_product(0, n + 1)
                pl.when(n == steps - 1)(lambda: load_start('m0'))
        return carry

    lax.fori_loop(0, steps, layer_one, 0)

    def mid_mate_copy(slot, part):
        return pltpu.make_async_remote_copy(
            src_ref=zp.at[1, 2 * part], dst_ref=m1r.at[slot, part],
            send_sem=m1_send.at[part], recv_sem=m1_recv.at[slot, part],
            device_id={'row': mate}, device_id_type=MESH)

    def mid_across_copy(slot):
        return pltpu.make_async_remote_copy(
            src_ref=zp.at[1, 1], dst_ref=myr.at[slot],
            send_sem=my_send, recv_sem=my_recv.at[slot],
            device_id={'row': across}, device_id_type=MESH)

    def mid_wait_send():
        for part in range(2):
            mid_mate_copy(0, part).wait_send()
        mid_across_copy(0).wait_send()

    def mid_product(t):
        slot = t % 3
        a = joined(hist.at[0, t + 1])
        b = joined(hist.at[1, steps - t])
        for idx in range(4):
            for s in range(SPLIT):
                z = dot(a, wx[0, idx, :, lanes_of(s)]) + dot(b, wx[1, idx, :, lanes_of(s)])
                if idx < 3:
                    zp[1, idx, s] = z
                else:
                    zm[t % 2, s] = z
            if idx % 2 == 0:
                mid_mate_copy(slot, idx // 2).start()
        mid_mate_copy(slot, 0).wait_recv()
        zp[1, 1] = zp[1, 1] + m1r[slot, 0]
        mid_across_copy(slot).start()

    def h2_copy(slot, i, p):
        return pltpu.make_async_remote_copy(
            src_ref=hsend.at[2], dst_ref=h2b.at[slot, p, row],
            send_sem=h2_send.at[i, p], recv_sem=h2_recv.at[slot, p, row],
            device_id={'col': far(i), 'row': (col + 2 * p) % n_row}, device_id_type=MESH)

    h2_stays = [row == (col + 2 * p) % n_row for p in range(2)]

    def h2_start(slot):
        for i in range(n_col):
            for p in range(2):
                pl.when(jnp.logical_not(h2_stays[p] & (far(i) == col)))(lambda i=i, p=p: h2_copy(slot, i, p).start())
        for p in range(2):
            @pl.when(h2_stays[p])
            def _(p=p):
                h2b[slot, p, row] = hsend[2]

    def h2_wait_send(slot):
        for i in range(n_col):
            for p in range(2):
                pl.when(jnp.logical_not(h2_stays[p] & (far(i) == col)))(
                    lambda i=i, p=p: h2_copy(slot, i, p).wait_send())

    def h2_wait_recv(slot, p):
        stays = (row + 2 * p) % n_row == col
        for j in range(n_row):
            def wait(j=j):
                pltpu.make_async_remote_copy(
                    src_ref=hsend.at[2], dst_ref=h2b.at[slot, p, j],
                    send_sem=h2_send.at[0, 0], recv_sem=h2_recv.at[slot, p, j],
                    device_id={'col': col, 'row': row}, device_id_type=MESH).wait_recv()
            pl.when(jnp.logical_not(stays & (row == j)))(wait)

    def distance(r):
        return (r - col) * (r - col)

    nearer = jnp.where(distance(row) < distance((row + 2) % n_row), 0, 1)

    for k in range(2):
        forward(2 * steps - 2 + k)
    for k in range(2):
        h_wait_send(k, hist.at[k, steps], steps % 2)
    for name in ('m0', 'm1'):
        load_wait(name)
    mid_product(1)
    for k in range(2):
        h_wait_recv(k, hist.at[k, steps], steps % 2)
    mid_wait_send()
    mid_product(0)
    h2_load.wait()
    h0_copy.wait()
    moved_rows = wh2.at[1, pl.ds(pl.multiple_of(data * half, 16), half)]
    came_rows = wh2.at[1, pl.ds(pl.multiple_of((1 - data) * half, 16), half)]
    pltpu.make_async_remote_copy(
        src_ref=moved_rows, dst_ref=moved_rows, send_sem=move_send, recv_sem=move_recv.at[0],
        device_id={'row': across}, device_id_type=MESH).wait_send()
    pltpu.make_async_remote_copy(
        src_ref=moved_rows, dst_ref=came_rows, send_sem=relay_send, recv_sem=relay_recv,
        device_id={'data': 1 - data}, device_id_type=MESH).wait()

    def layer_two(n, carry):
        slot = n % 2

        parts = ((0, 1 - core), (3, core))

        def cols_of(part, s):
            return pl.ds(pl.multiple_of(part * width + s * part_n, LANES), part_n)

        pl.when(n > 0)(lambda: h2_wait_recv(slot, nearer))
        a = joined(h2b.at[slot, nearer])
        for idx, part in parts:
            for s in range(SPLIT):
                zp[0, idx, s] = dot(a, wh2[nearer, :, cols_of(part, s)])
        pl.when(n > 0)(lambda: h2_wait_recv(slot, 1 - nearer))
        a = joined(h2b.at[slot, 1 - nearer])
        todo = []

        def finish(idx, s, z):
            zp[0, idx, s] = zp[0, idx, s] + z
            if idx == 0:
                mate_copy(0, slot, 0, s).start()

        for idx, part in parts:
            for s in range(SPLIT):
                todo.append((idx, s, dot(a, wh2[1 - nearer, :, cols_of(part, s)])))
                if len(todo) > 1:
                    finish(*todo.pop(0))
        finish(*todo.pop(0))
        for s in range(SPLIT):
            mate_copy(0, slot, 0, s).wait_recv()
        mid_slot = n % 3
        mid_mate_copy(mid_slot, 1).wait_recv()
        mid_across_copy(mid_slot).wait_recv()
        h = gates(2, b2_ref, 0, (zp.at[0, 3], p1r.at[0, slot, 0], zm.at[slot],
                                 m1r.at[mid_slot, 1], myr.at[mid_slot]))
        for s in range(SPLIT):
            mate_copy(0, slot, 0, s).wait_send()

        @pl.when(n > 0)
        def _():
            h2_wait_send(slot)
        hsend[2] = h
        out_ref[n] = h

        @pl.when(n < steps - 1)
        def _():
            h2_start(1 - slot)

        @pl.when(n < steps - 2)
        def _():
            mid_wait_send()
            mid_product(n + 2)
        return carry

    lax.fori_loop(0, steps, layer_two, 0)
    mid_wait_send()
    for k in range(3):
        c_out[k] = moved(c_ref[k], sel[...])


def solution(mesh):
    n_data = mesh.shape['data']
    n_row = mesh.shape['row']
    n_col = mesh.shape['col']
    spec_seq = P(None, 'data', 'row')
    spec_weight = P(None, 'row', 'col')
    spec_out = P(None, 'data', ('col', 'row'))

    def local(x_rows, w_x1, w_h1, b_1, w_x2, w_h2, b_2, h_zero, c_zero):
        steps, batch, d_row = x_rows.shape
        unit_n = d_row // n_col
        width = 4 * unit_n
        vmem = pl.BlockSpec(memory_space=pltpu.VMEM)
        hbm = pl.BlockSpec(memory_space=pl.ANY)
        dma = pltpu.SemaphoreType.DMA
        return pl.pallas_call(
            functools.partial(lstm_kernel, steps, n_data, n_row, n_col),
            out_shape=(jax.ShapeDtypeStruct((steps, batch, unit_n), BF16),
                       jax.ShapeDtypeStruct((3, batch, unit_n), F32)),
            in_specs=[vmem, hbm, hbm, hbm, hbm, vmem, vmem, vmem, vmem],
            out_specs=(vmem, vmem),
            scratch_shapes=[
                pltpu.VMEM((2, 4, d_row, width), BF16),
                pltpu.VMEM((2, 4, d_row, width), BF16),
                pltpu.VMEM((2, d_row, 2 * width), BF16),
                pltpu.VMEM((2, steps + 1, n_row, batch, unit_n), BF16),
                pltpu.VMEM((2, 2, n_row, batch, unit_n), BF16),
                pltpu.VMEM((2, 4, SPLIT, batch, width // SPLIT), F32),
                pltpu.VMEM((2, 2, 2, SPLIT, batch, width // SPLIT), F32),
                pltpu.VMEM((2, 2, SPLIT, batch, width // SPLIT), F32),
                pltpu.VMEM((2, SPLIT, batch, width // SPLIT), F32),
                pltpu.VMEM((3, 2, SPLIT, batch, width // SPLIT), F32),
                pltpu.VMEM((3, SPLIT, batch, width // SPLIT), F32),
                pltpu.VMEM((3, batch, unit_n), BF16),
                pltpu.VMEM((width, unit_n), BF16),
                pltpu.VMEM((unit_n, width), BF16),
                pltpu.VMEM((3, batch, unit_n), F32),
                pltpu.VMEM((3, batch, width), F32),
                dma((2,)),
                dma((7, 4)), dma((2, 2, SPLIT)), dma((2, 2, 2, SPLIT)), dma((2, SPLIT)), dma((2, 2, SPLIT)),
                dma((2,)), dma((3, 2)), dma, dma((3,)),
                dma((2, n_col)), dma((2, 2, n_row)), dma((n_col, 2)), dma((2, 2, n_row)),
                dma((2,)), dma, dma((8,)), dma, dma,
            ],
            compiler_params=pltpu.CompilerParams(
                collective_id=0, has_side_effects=True, vmem_limit_bytes=60 * 1024 * 1024),
        )(x_rows, w_x1, w_h1, w_x2, w_h2, b_1, b_2[None], h_zero, c_zero)

    return jax.shard_map(local, mesh=mesh,
                         in_specs=(spec_seq, spec_weight, spec_weight, P(None, 'col'), spec_weight,
                                   P('row', 'col'), P('col'), spec_seq, spec_seq),
                         out_specs=(spec_out, spec_out), check_vma=False)
```

```python
import functools

import jax
import jax.numpy as jnp
from jax import lax
from jax.experimental import pallas as pl
from jax.experimental.pallas import tpu as pltpu
from jax.sharding import PartitionSpec as P

MESH = pl.DeviceIdType.MESH
F32 = jnp.float32
BF16 = jnp.bfloat16
LANES = 128
SPLIT = 2


def lstm_kernel(steps, n_data, n_row, n_col,
                x_ref, wx1_hbm, wh1_hbm, wx2_hbm, wh2_hbm, b1_ref, b2_ref, h0_ref, c0_ref,
                out_ref, c_out,
                wx, wh, wh2, hist, h2b, zp, p1r, yr, zm, m1r, myr, hsend, sel, spread, c_own, c_ref,
                c_sem, w_sem, p1_send, p1_recv, y_send, y_recv, m1_send, m1_recv, my_send, my_recv,
                h_send, h_recv, h2_send, h2_recv, h0_sem, move_send, move_recv, relay_send, relay_recv):
    data = lax.axis_index('data')
    row = lax.axis_index('row')
    col = lax.axis_index('col')
    batch, d_row = x_ref.shape[1], x_ref.shape[2]
    unit_n = d_row // n_col
    width = 4 * unit_n
    part_n = width // SPLIT
    core = row % 2
    mate = row + 1 - 2 * core
    across = (row + 2) % 4
    order = (3 - row, across, mate, row)

    def weight_copy(src, dst, idx, sem):
        cols = pl.ds(pl.multiple_of(order[idx] * width, LANES), width)
        return pltpu.make_async_copy(src.at[:, cols], dst.at[idx], w_sem.at[sem, idx])

    loads = {'x0': (wx1_hbm.at[0], wx.at[0], 0), 'h0': (wh1_hbm.at[0], wh.at[0], 1),
             'x1': (wx1_hbm.at[1], wx.at[1], 2), 'h1': (wh1_hbm.at[1], wh.at[1], 3),
             'm0': (wx2_hbm.at[0], wx.at[0], 4), 'm1': (wx2_hbm.at[1], wx.at[1], 5)}

    def load_start(name):
        for idx in range(4):
            src, dst, sem = loads[name]
            weight_copy(src, dst, idx, sem).start()

    def load_wait(name):
        for idx in range(4):
            src, dst, sem = loads[name]
            weight_copy(src, dst, idx, sem).wait()

    for name in ('x0', 'h0', 'x1', 'h1'):
        load_start(name)

    half = d_row // 2
    piece = half // (2 * steps)
    own_cols = pl.ds(pl.multiple_of(row // 2 * (2 * width), LANES), 2 * width)
    far_cols = pl.ds(pl.multiple_of((1 - row // 2) * (2 * width), LANES), 2 * width)
    h2_load = pltpu.make_async_copy(wh2_hbm.at[:, own_cols], wh2.at[0], w_sem.at[6, 0])
    h2_load.start()

    def piece_rows(part, p):
        return pl.ds(pl.multiple_of(part * half + p * piece, 16), piece)

    def move_copy(p):
        rows = piece_rows(data, p)
        return pltpu.make_async_remote_copy(
            src_ref=wh2_hbm.at[rows, far_cols], dst_ref=wh2.at[1, rows],
            send_sem=move_send, recv_sem=move_recv.at[p % 8],
            device_id={'row': across}, device_id_type=MESH)

    def relay_copy(p):
        rows = piece_rows(data, p)
        return pltpu.make_async_remote_copy(
            src_ref=wh2.at[1, rows], dst_ref=wh2.at[1, rows],
            send_sem=relay_send, recv_sem=relay_recv,
            device_id={'data': 1 - data}, device_id_type=MESH)

    def forward(p):
        move_copy(p).wait_recv()
        relay_copy(p).start()

    barrier = pltpu.get_barrier_semaphore()
    for dc in range(n_col):
        for dr in range(n_row):
            if dc or dr:
                pl.semaphore_signal(barrier, inc=1, device_id_type=MESH,
                                    device_id={'col': (col + dc) % n_col, 'row': (row + dr) % n_row})
    pl.semaphore_signal(barrier, inc=1, device_id_type=MESH, device_id={'data': 1 - data})

    rr = lax.broadcasted_iota(jnp.int32, (width, unit_n), 0)
    cc = lax.broadcasted_iota(jnp.int32, (width, unit_n), 1)
    sel[...] = jnp.where(rr == 4 * cc, 1.0, 0.0).astype(BF16)
    for k in range(2):
        for j in range(n_row):
            hist[k, 0, j] = h0_ref[k, :, j * unit_n:(j + 1) * unit_n].astype(BF16)
    for j in range(n_row):
        h2b[0, 0, j] = h0_ref[2, :, j * unit_n:(j + 1) * unit_n].astype(BF16)
    rr = lax.broadcasted_iota(jnp.int32, (unit_n, width), 0)
    cc = lax.broadcasted_iota(jnp.int32, (unit_n, width), 1)
    spread[...] = jnp.where(rr == cc // 4, 1.0, 0.0).astype(BF16)

    own_stays = row == col
    c_part = pl.ds(pl.multiple_of(col * unit_n, LANES), unit_n)
    c_copy = pltpu.make_async_remote_copy(
        src_ref=c0_ref.at[:, :, c_part], dst_ref=c_own, send_sem=c_sem.at[0], recv_sem=c_sem.at[1],
        device_id={'col': row, 'row': col}, device_id_type=MESH)
    pl.semaphore_wait(barrier, n_col * n_row)

    @pl.when(jnp.logical_not(own_stays))
    def _():
        c_copy.start()

    @pl.when(own_stays)
    def _():
        c_own[...] = c0_ref[:, :, c_part]

    h0_copy = pltpu.make_async_remote_copy(
        src_ref=h2b.at[0, 0], dst_ref=h2b.at[0, 1], send_sem=h0_sem.at[0], recv_sem=h0_sem.at[1],
        device_id={'row': across}, device_id_type=MESH)
    h0_copy.start()

    def dot(a, w):
        return jnp.dot(a, w, preferred_element_type=F32)

    def lanes_of(s):
        return slice(s * part_n, (s + 1) * part_n)

    def moved(a, m):
        a = a * 0.5
        top = a.astype(BF16)
        rest = a - top.astype(F32)
        mid = rest.astype(BF16)
        low = (rest - mid.astype(F32)).astype(BF16)
        parts = dot(jnp.concatenate([top, mid, low], axis=0), m)
        return ((parts[:batch] + parts[batch:2 * batch]) + parts[2 * batch:]) * 2.0

    def joined(blocks):
        return jnp.concatenate([blocks[j] for j in range(n_row)], axis=1)

    def input_product(k, t):
        a = x_ref[t]
        for idx in range(4):
            for s in range(SPLIT):
                zp[k, idx, s] = dot(a, wx[k, idx, :, lanes_of(s)])

    load_wait('x0')
    input_product(0, 0)
    load_wait('h0')

    @pl.when(jnp.logical_not(own_stays))
    def _():
        c_copy.wait()
    for k in range(3):
        c_ref[k] = moved(c_own[k], spread[...])

    def mate_copy(k, slot, part, s):
        return pltpu.make_async_remote_copy(
            src_ref=zp.at[k, 2 * part, s], dst_ref=p1r.at[k, slot, part, s],
            send_sem=p1_send.at[k, part, s], recv_sem=p1_recv.at[k, slot, part, s],
            device_id={'row': mate}, device_id_type=MESH)

    def across_copy(k, slot, s):
        return pltpu.make_async_remote_copy(
            src_ref=zp.at[k, 1, s], dst_ref=yr.at[k, slot, s],
            send_sem=y_send.at[k, s], recv_sem=y_recv.at[k, slot, s],
            device_id={'row': across}, device_id_type=MESH)

    def far(i):
        return (n_col - 1 - i) + (2 * i - (n_col - 1)) * (col // (n_col // 2))

    def h_copy(k, dst, slot, i):
        return pltpu.make_async_remote_copy(
            src_ref=hsend.at[k], dst_ref=dst.at[row],
            send_sem=h_send.at[k, i], recv_sem=h_recv.at[k, slot, row],
            device_id={'col': far(i), 'row': col}, device_id_type=MESH)

    def h_start(k, dst, slot):
        for i in range(n_col):
            pl.when(jnp.logical_not(own_stays & (far(i) == col)))(lambda i=i: h_copy(k, dst, slot, i).start())

        @pl.when(own_stays)
        def _():
            dst[row] = hsend[k]

    def h_wait_send(k, dst, slot):
        for i in range(n_col):
            pl.when(jnp.logical_not(own_stays & (far(i) == col)))(lambda i=i: h_copy(k, dst, slot, i).wait_send())

    def h_wait_recv(k, dst, slot):
        for j in range(n_row):
            def wait(j=j):
                pltpu.make_async_remote_copy(
                    src_ref=hsend.at[k], dst_ref=dst.at[j],
                    send_sem=h_send.at[k, 0], recv_sem=h_recv.at[k, slot, j],
                    device_id={'col': col, 'row': row}, device_id_type=MESH).wait_recv()
            pl.when(jnp.logical_not(own_stays & (row == j)))(wait)

    def head(k, slot, blocks, w_rec):
        a = joined(blocks)
        todo = []

        def finish(idx, s, z):
            zp[k, idx, s] = zp[k, idx, s] + z
            if idx % 2 == 0:
                mate_copy(k, slot, idx // 2, s).start()

        for idx in range(4):
            for s in range(SPLIT):
                todo.append((idx, s, dot(a, w_rec[idx, :, lanes_of(s)])))
                if len(todo) > 1:
                    finish(*todo.pop(0))
            if idx == 2:
                finish(*todo.pop(0))
                pl.when(core == 0)(lambda: middle(k, slot))
        finish(*todo.pop(0))
        if k:
            pl.when(core != 0)(lambda: middle(k, slot))

    def middle(k, slot):
        for s in range(SPLIT):
            mate_copy(k, slot, 0, s).wait_recv()
            zp[k, 1, s] = zp[k, 1, s] + p1r[k, slot, 0, s]
            across_copy(k, slot, s).start()

    def gates(cell, bias_ref, bias_row, addends):
        gate = lax.broadcasted_iota(jnp.int32, (batch, LANES), 1) % 4
        scale = jnp.where(gate == 2, 1.0, 0.5)
        shift = jnp.where(gate == 2, 0.0, 0.5)
        pieces = []
        for p in range(width // LANES):
            lanes = slice(p * LANES, (p + 1) * LANES)
            z = bias_ref[bias_row:bias_row + 1, pl.ds(pl.multiple_of(row * width, LANES) + p * LANES, LANES)]
            for a in addends:
                z = z + a[p * LANES // part_n, :, pl.ds(p * LANES % part_n, LANES)]
            act = jnp.tanh(z * scale) * scale + shift
            f = pltpu.roll(act, LANES - 1, 1)
            g = pltpu.roll(act, LANES - 2, 1)
            o = pltpu.roll(act, LANES - 3, 1)
            c_new = f * c_ref[cell, :, lanes] + act * g
            c_ref[cell, :, lanes] = c_new
            pieces.append((o * jnp.tanh(c_new)).astype(BF16))
        return dot(jnp.concatenate(pieces, axis=1), sel[...]).astype(BF16)

    def gates_one(k, slot):
        for s in range(SPLIT):
            mate_copy(k, slot, 1, s).wait_recv()
            across_copy(k, slot, s).wait_recv()
        h = gates(k, b1_ref, k, (zp.at[k, 3], p1r.at[k, slot, 1], yr.at[k, slot]))
        for s in range(SPLIT):
            for part in range(2):
                mate_copy(k, slot, part, s).wait_send()
            across_copy(k, slot, s).wait_send()
        return h

    def layer_one(n, carry):
        slot = n % 2
        for k in range(2):
            if k == 1:
                pl.when(n == 0)(lambda: load_wait('x1'))
                input_product(1, steps - 1 - n)
                pl.when(core != 0)(lambda: middle(0, slot))
                pl.when(n == 0)(lambda: load_wait('h1'))
                pl.when(n == steps - 1)(lambda: load_start('m1'))

            @pl.when(n > 0)
            def _(k=k):
                h_wait_recv(k, hist.at[k, n], slot)
            head(k, slot, hist.at[k, n], wh.at[k])
        for k in range(2):
            h = gates_one(k, slot)

            @pl.when(n > 0)
            def _(k=k):
                h_wait_send(k, hist.at[k, n], slot)
            hsend[k] = h
            h_start(k, hist.at[k, n + 1], (n + 1) % 2)

            @pl.when(n > 0)
            def _(k=k):
                forward(2 * n - 2 + k)

            if k == 0:
                move_copy(2 * n).start()
                move_copy(2 * n + 1).start()

            if k == 0:
                @pl.when(n < steps - 1)
                def _():
                    input_product(0, n + 1)
                pl.when(n == steps - 1)(lambda: load_start('m0'))
        return carry

    lax.fori_loop(0, steps, layer_one, 0)

    def mid_mate_copy(slot, part):
        return pltpu.make_async_remote_copy(
            src_ref=zp.at[1, 2 * part], dst_ref=m1r.at[slot, part],
            send_sem=m1_send.at[part], recv_sem=m1_recv.at[slot, part],
            device_id={'row': mate}, device_id_type=MESH)

    def mid_across_copy(slot):
        return pltpu.make_async_remote_copy(
            src_ref=zp.at[1, 1], dst_ref=myr.at[slot],
            send_sem=my_send, recv_sem=my_recv.at[slot],
            device_id={'row': across}, device_id_type=MESH)

    def mid_wait_send():
        for part in range(2):
            mid_mate_copy(0, part).wait_send()
        mid_across_copy(0).wait_send()

    def mid_product(t):
        slot = t % 3
        a = joined(hist.at[0, t + 1])
        b = joined(hist.at[1, steps - t])
        for idx in range(4):
            for s in range(SPLIT):
                z = dot(a, wx[0, idx, :, lanes_of(s)]) + dot(b, wx[1, idx, :, lanes_of(s)])
                if idx < 3:
                    zp[1, idx, s] = z
                else:
                    zm[t % 2, s] = z
            if idx % 2 == 0:
                mid_mate_copy(slot, idx // 2).start()
        mid_mate_copy(slot, 0).wait_recv()
        zp[1, 1] = zp[1, 1] + m1r[slot, 0]
        mid_across_copy(slot).start()

    def h2_copy(slot, i, p):
        return pltpu.make_async_remote_copy(
            src_ref=hsend.at[2], dst_ref=h2b.at[slot, p, row],
            send_sem=h2_send.at[i, p], recv_sem=h2_recv.at[slot, p, row],
            device_id={'col': far(i), 'row': (col + 2 * p) % n_row}, device_id_type=MESH)

    h2_stays = [row == (col + 2 * p) % n_row for p in range(2)]

    cross = 1 - (col // 2 - row // 2) * (col // 2 - row // 2)

    def h2_start(slot):
        for i in range(n_col):
            for q in range(2):
                p = (q + cross) % 2
                stays = (row == (col + 2 * p) % n_row) & (far(i) == col)
                pl.when(jnp.logical_not(stays))(lambda i=i, p=p: h2_copy(slot, i, p).start())
        for p in range(2):
            @pl.when(h2_stays[p])
            def _(p=p):
                h2b[slot, p, row] = hsend[2]

    def h2_wait_send(slot):
        for i in range(n_col):
            for p in range(2):
                pl.when(jnp.logical_not(h2_stays[p] & (far(i) == col)))(
                    lambda i=i, p=p: h2_copy(slot, i, p).wait_send())

    def h2_wait_recv(slot, p):
        stays = (row + 2 * p) % n_row == col
        for j in range(n_row):
            def wait(j=j):
                pltpu.make_async_remote_copy(
                    src_ref=hsend.at[2], dst_ref=h2b.at[slot, p, j],
                    send_sem=h2_send.at[0, 0], recv_sem=h2_recv.at[slot, p, j],
                    device_id={'col': col, 'row': row}, device_id_type=MESH).wait_recv()
            pl.when(jnp.logical_not(stays & (row == j)))(wait)

    def distance(r):
        return (r - col) * (r - col)

    nearer = jnp.where(distance(row) < distance((row + 2) % n_row), 0, 1)

    for k in range(2):
        forward(2 * steps - 2 + k)
    for k in range(2):
        h_wait_send(k, hist.at[k, steps], steps % 2)
    for name in ('m0', 'm1'):
        load_wait(name)
    mid_product(1)
    for k in range(2):
        h_wait_recv(k, hist.at[k, steps], steps % 2)
    mid_wait_send()
    mid_product(0)
    h2_load.wait()
    h0_copy.wait()
    moved_rows = wh2.at[1, pl.ds(pl.multiple_of(data * half, 16), half)]
    came_rows = wh2.at[1, pl.ds(pl.multiple_of((1 - data) * half, 16), half)]
    pltpu.make_async_remote_copy(
        src_ref=moved_rows, dst_ref=moved_rows, send_sem=move_send, recv_sem=move_recv.at[0],
        device_id={'row': across}, device_id_type=MESH).wait_send()
    pltpu.make_async_remote_copy(
        src_ref=moved_rows, dst_ref=came_rows, send_sem=relay_send, recv_sem=relay_recv,
        device_id={'data': 1 - data}, device_id_type=MESH).wait()

    def layer_two(n, carry):
        slot = n % 2

        parts = ((0, 1 - core), (3, core))

        def cols_of(part, s):
            return pl.ds(pl.multiple_of(part * width + s * part_n, LANES), part_n)

        pl.when(n > 0)(lambda: h2_wait_recv(slot, nearer))
        a = joined(h2b.at[slot, nearer])
        for idx, part in parts:
            for s in range(SPLIT):
                zp[0, idx, s] = dot(a, wh2[nearer, :, cols_of(part, s)])
        pl.when(n > 0)(lambda: h2_wait_recv(slot, 1 - nearer))
        a = joined(h2b.at[slot, 1 - nearer])
        todo = []

        def finish(idx, s, z):
            zp[0, idx, s] = zp[0, idx, s] + z
            if idx == 0:
                mate_copy(0, slot, 0, s).start()

        for idx, part in parts:
            for s in range(SPLIT):
                todo.append((idx, s, dot(a, wh2[1 - nearer, :, cols_of(part, s)])))
                if len(todo) > 1:
                    finish(*todo.pop(0))
        finish(*todo.pop(0))
        for s in range(SPLIT):
            mate_copy(0, slot, 0, s).wait_recv()
        mid_slot = n % 3
        mid_mate_copy(mid_slot, 1).wait_recv()
        mid_across_copy(mid_slot).wait_recv()
        h = gates(2, b2_ref, 0, (zp.at[0, 3], p1r.at[0, slot, 0], zm.at[slot],
                                 m1r.at[mid_slot, 1], myr.at[mid_slot]))
        for s in range(SPLIT):
            mate_copy(0, slot, 0, s).wait_send()

        @pl.when(n > 0)
        def _():
            h2_wait_send(slot)
        hsend[2] = h
        out_ref[n] = h

        @pl.when(n < steps - 1)
        def _():
            h2_start(1 - slot)

        @pl.when(n < steps - 2)
        def _():
            mid_wait_send()
            mid_product(n + 2)
        return carry

    lax.fori_loop(0, steps, layer_two, 0)
    mid_wait_send()
    for k in range(3):
        c_out[k] = moved(c_ref[k], sel[...])


def solution(mesh):
    n_data = mesh.shape['data']
    n_row = mesh.shape['row']
    n_col = mesh.shape['col']
    spec_seq = P(None, 'data', 'row')
    spec_weight = P(None, 'row', 'col')
    spec_out = P(None, 'data', ('col', 'row'))

    def local(x_rows, w_x1, w_h1, b_1, w_x2, w_h2, b_2, h_zero, c_zero):
        steps, batch, d_row = x_rows.shape
        unit_n = d_row // n_col
        width = 4 * unit_n
        vmem = pl.BlockSpec(memory_space=pltpu.VMEM)
        hbm = pl.BlockSpec(memory_space=pl.ANY)
        dma = pltpu.SemaphoreType.DMA
        out = pl.pallas_call(
            functools.partial(lstm_kernel, steps, n_data, n_row, n_col),
            out_shape=(jax.ShapeDtypeStruct((steps, batch, unit_n), BF16),
                       jax.ShapeDtypeStruct((3, batch, unit_n), F32)),
            in_specs=[vmem, hbm, hbm, hbm, hbm, vmem, vmem, vmem, vmem],
            out_specs=(vmem, vmem),
            scratch_shapes=[
                pltpu.VMEM((2, 4, d_row, width), BF16),
                pltpu.VMEM((2, 4, d_row, width), BF16),
                pltpu.VMEM((2, d_row, 2 * width), BF16),
                pltpu.VMEM((2, steps + 1, n_row, batch, unit_n), BF16),
                pltpu.VMEM((2, 2, n_row, batch, unit_n), BF16),
                pltpu.VMEM((2, 4, SPLIT, batch, width // SPLIT), F32),
                pltpu.VMEM((2, 2, 2, SPLIT, batch, width // SPLIT), F32),
                pltpu.VMEM((2, 2, SPLIT, batch, width // SPLIT), F32),
                pltpu.VMEM((2, SPLIT, batch, width // SPLIT), F32),
                pltpu.VMEM((3, 2, SPLIT, batch, width // SPLIT), F32),
                pltpu.VMEM((3, SPLIT, batch, width // SPLIT), F32),
                pltpu.VMEM((3, batch, unit_n), BF16),
                pltpu.VMEM((width, unit_n), BF16),
                pltpu.VMEM((unit_n, width), BF16),
                pltpu.VMEM((3, batch, unit_n), F32),
                pltpu.VMEM((3, batch, width), F32),
                dma((2,)),
                dma((7, 4)), dma((2, 2, SPLIT)), dma((2, 2, 2, SPLIT)), dma((2, SPLIT)), dma((2, 2, SPLIT)),
                dma((2,)), dma((3, 2)), dma, dma((3,)),
                dma((2, n_col)), dma((2, 2, n_row)), dma((n_col, 2)), dma((2, 2, n_row)),
                dma((2,)), dma, dma((8,)), dma, dma,
            ],
            compiler_params=pltpu.CompilerParams(
                collective_id=0, has_side_effects=True, vmem_limit_bytes=60 * 1024 * 1024),
        )(x_rows, w_x1, w_h1, w_x2, w_h2, b_1, b_2[None], h_zero, c_zero)

        def copy_out(a_ref, b_ref, a_out, b_out):
            a_out[...] = a_ref[...]
            b_out[...] = b_ref[...]

        return pl.pallas_call(
            copy_out, in_specs=[vmem, vmem], out_specs=(vmem, vmem),
            out_shape=(jax.ShapeDtypeStruct((steps, batch, unit_n), BF16),
                       jax.ShapeDtypeStruct((3, batch, unit_n), F32)))(*out)

    return jax.shard_map(local, mesh=mesh,
                         in_specs=(spec_seq, spec_weight, spec_weight, P(None, 'col'), spec_weight,
                                   P('row', 'col'), P('col'), spec_seq, spec_seq),
                         out_specs=(spec_out, spec_out), check_vma=False)
```

```python
import functools

import jax
import jax.numpy as jnp
from jax import lax
from jax.experimental import pallas as pl
from jax.experimental.pallas import tpu as pltpu
from jax.sharding import PartitionSpec as P

MESH = pl.DeviceIdType.MESH
F32 = jnp.float32
BF16 = jnp.bfloat16
LANES = 128
SPLIT = 2


def lstm_kernel(steps, n_data, n_row, n_col,
                x_ref, wx1_hbm, wh1_hbm, wx2_hbm, wh2_hbm, b1_ref, b2_ref, h0_ref, c0_ref,
                out_ref, c_out,
                wx, wh, wh2, hist, h2b, zp, p1r, yr, zm, m1r, myr, hsend, sel, spread, c_own, c_ref,
                c_sem, w_sem, p1_send, p1_recv, y_send, y_recv, m1_send, m1_recv, my_send, my_recv,
                h_send, h_recv, h2_send, h2_recv, h0_sem, move_send, move_recv, relay_send, relay_recv):
    data = lax.axis_index('data')
    row = lax.axis_index('row')
    col = lax.axis_index('col')
    batch, d_row = x_ref.shape[1], x_ref.shape[2]
    unit_n = d_row // n_col
    width = 4 * unit_n
    part_n = width // SPLIT
    core = row % 2
    mate = row + 1 - 2 * core
    across = (row + 2) % 4
    order = (3 - row, across, mate, row)

    def weight_copy(src, dst, idx, sem):
        cols = pl.ds(pl.multiple_of(order[idx] * width, LANES), width)
        return pltpu.make_async_copy(src.at[:, cols], dst.at[idx], w_sem.at[sem, idx])

    loads = {'x0': (wx1_hbm.at[0], wx.at[0], 0), 'h0': (wh1_hbm.at[0], wh.at[0], 1),
             'x1': (wx1_hbm.at[1], wx.at[1], 2), 'h1': (wh1_hbm.at[1], wh.at[1], 3),
             'm0': (wx2_hbm.at[0], wx.at[0], 4), 'm1': (wx2_hbm.at[1], wx.at[1], 5)}

    def load_start(name):
        for idx in range(4):
            src, dst, sem = loads[name]
            weight_copy(src, dst, idx, sem).start()

    def load_wait(name):
        for idx in range(4):
            src, dst, sem = loads[name]
            weight_copy(src, dst, idx, sem).wait()

    for name in ('x0', 'h0', 'x1', 'h1'):
        load_start(name)

    half = d_row // 2
    piece = half // (2 * steps)
    own_cols = pl.ds(pl.multiple_of(row // 2 * (2 * width), LANES), 2 * width)
    far_cols = pl.ds(pl.multiple_of((1 - row // 2) * (2 * width), LANES), 2 * width)
    h2_load = pltpu.make_async_copy(wh2_hbm.at[:, own_cols], wh2.at[0], w_sem.at[6, 0])
    h2_load.start()

    def piece_rows(part, p):
        return pl.ds(pl.multiple_of(part * half + p * piece, 16), piece)

    def move_copy(p):
        rows = piece_rows(data, p)
        return pltpu.make_async_remote_copy(
            src_ref=wh2_hbm.at[rows, far_cols], dst_ref=wh2.at[1, rows],
            send_sem=move_send, recv_sem=move_recv.at[p % 8],
            device_id={'row': across}, device_id_type=MESH)

    def relay_copy(p):
        rows = piece_rows(data, p)
        return pltpu.make_async_remote_copy(
            src_ref=wh2.at[1, rows], dst_ref=wh2.at[1, rows],
            send_sem=relay_send, recv_sem=relay_recv,
            device_id={'data': 1 - data}, device_id_type=MESH)

    def forward(p):
        move_copy(p).wait_recv()
        relay_copy(p).start()

    barrier = pltpu.get_barrier_semaphore()
    for dc in range(n_col):
        for dr in range(n_row):
            if dc or dr:
                pl.semaphore_signal(barrier, inc=1, device_id_type=MESH,
                                    device_id={'col': (col + dc) % n_col, 'row': (row + dr) % n_row})
    pl.semaphore_signal(barrier, inc=1, device_id_type=MESH, device_id={'data': 1 - data})

    rr = lax.broadcasted_iota(jnp.int32, (width, unit_n), 0)
    cc = lax.broadcasted_iota(jnp.int32, (width, unit_n), 1)
    sel[...] = jnp.where(rr == 4 * cc, 1.0, 0.0).astype(BF16)
    for k in range(2):
        for j in range(n_row):
            hist[k, 0, j] = h0_ref[k, :, j * unit_n:(j + 1) * unit_n].astype(BF16)
    for j in range(n_row):
        h2b[0, 0, j] = h0_ref[2, :, j * unit_n:(j + 1) * unit_n].astype(BF16)
    rr = lax.broadcasted_iota(jnp.int32, (unit_n, width), 0)
    cc = lax.broadcasted_iota(jnp.int32, (unit_n, width), 1)
    spread[...] = jnp.where(rr == cc // 4, 1.0, 0.0).astype(BF16)

    own_stays = row == col
    c_part = pl.ds(pl.multiple_of(col * unit_n, LANES), unit_n)
    c_copy = pltpu.make_async_remote_copy(
        src_ref=c0_ref.at[:, :, c_part], dst_ref=c_own, send_sem=c_sem.at[0], recv_sem=c_sem.at[1],
        device_id={'col': row, 'row': col}, device_id_type=MESH)
    pl.semaphore_wait(barrier, n_col * n_row)

    @pl.when(jnp.logical_not(own_stays))
    def _():
        c_copy.start()

    @pl.when(own_stays)
    def _():
        c_own[...] = c0_ref[:, :, c_part]

    h0_copy = pltpu.make_async_remote_copy(
        src_ref=h2b.at[0, 0], dst_ref=h2b.at[0, 1], send_sem=h0_sem.at[0], recv_sem=h0_sem.at[1],
        device_id={'row': across}, device_id_type=MESH)
    h0_copy.start()

    def dot(a, w):
        return jnp.dot(a, w, preferred_element_type=F32)

    def lanes_of(s):
        return slice(s * part_n, (s + 1) * part_n)

    def moved(a, m):
        a = a * 0.5
        top = a.astype(BF16)
        rest = a - top.astype(F32)
        mid = rest.astype(BF16)
        low = (rest - mid.astype(F32)).astype(BF16)
        parts = dot(jnp.concatenate([top, mid, low], axis=0), m)
        return ((parts[:batch] + parts[batch:2 * batch]) + parts[2 * batch:]) * 2.0

    def joined(blocks):
        return jnp.concatenate([blocks[j] for j in range(n_row)], axis=1)

    def input_product(k, t):
        a = x_ref[t]
        for idx in range(4):
            for s in range(SPLIT):
                zp[k, idx, s] = dot(a, wx[k, idx, :, lanes_of(s)])

    load_wait('x0')
    input_product(0, 0)

    @pl.when(jnp.logical_not(own_stays))
    def _():
        c_copy.wait()
    for k in range(3):
        c_ref[k] = moved(c_own[k], spread[...])
    load_wait('h0')

    def mate_copy(k, slot, part, s):
        return pltpu.make_async_remote_copy(
            src_ref=zp.at[k, 2 * part, s], dst_ref=p1r.at[k, slot, part, s],
            send_sem=p1_send.at[k, part, s], recv_sem=p1_recv.at[k, slot, part, s],
            device_id={'row': mate}, device_id_type=MESH)

    def across_copy(k, slot, s):
        return pltpu.make_async_remote_copy(
            src_ref=zp.at[k, 1, s], dst_ref=yr.at[k, slot, s],
            send_sem=y_send.at[k, s], recv_sem=y_recv.at[k, slot, s],
            device_id={'row': across}, device_id_type=MESH)

    def far(i):
        return (n_col - 1 - i) + (2 * i - (n_col - 1)) * (col // (n_col // 2))

    def h_copy(k, dst, slot, i):
        return pltpu.make_async_remote_copy(
            src_ref=hsend.at[k], dst_ref=dst.at[row],
            send_sem=h_send.at[k, i], recv_sem=h_recv.at[k, slot, row],
            device_id={'col': far(i), 'row': col}, device_id_type=MESH)

    def h_start(k, dst, slot):
        for i in range(n_col):
            pl.when(jnp.logical_not(own_stays & (far(i) == col)))(lambda i=i: h_copy(k, dst, slot, i).start())

        @pl.when(own_stays)
        def _():
            dst[row] = hsend[k]

    def h_wait_send(k, dst, slot):
        for i in range(n_col):
            pl.when(jnp.logical_not(own_stays & (far(i) == col)))(lambda i=i: h_copy(k, dst, slot, i).wait_send())

    def h_wait_recv(k, dst, slot):
        for j in range(n_row):
            def wait(j=j):
                pltpu.make_async_remote_copy(
                    src_ref=hsend.at[k], dst_ref=dst.at[j],
                    send_sem=h_send.at[k, 0], recv_sem=h_recv.at[k, slot, j],
                    device_id={'col': col, 'row': row}, device_id_type=MESH).wait_recv()
            pl.when(jnp.logical_not(own_stays & (row == j)))(wait)

    def head(k, slot, blocks, w_rec):
        a = joined(blocks)
        todo = []

        def finish(idx, s, z):
            zp[k, idx, s] = zp[k, idx, s] + z
            if idx % 2 == 0:
                mate_copy(k, slot, idx // 2, s).start()

        for idx in range(4):
            for s in range(SPLIT):
                todo.append((idx, s, dot(a, w_rec[idx, :, lanes_of(s)])))
                if len(todo) > 1:
                    finish(*todo.pop(0))
            if idx == 2:
                finish(*todo.pop(0))
                pl.when(core == 0)(lambda: middle(k, slot))
        finish(*todo.pop(0))
        if k:
            pl.when(core != 0)(lambda: middle(k, slot))

    def middle(k, slot):
        for s in range(SPLIT):
            mate_copy(k, slot, 0, s).wait_recv()
            zp[k, 1, s] = zp[k, 1, s] + p1r[k, slot, 0, s]
            across_copy(k, slot, s).start()

    def gates(cell, bias_ref, bias_row, addends):
        gate = lax.broadcasted_iota(jnp.int32, (batch, LANES), 1) % 4
        scale = jnp.where(gate == 2, 1.0, 0.5)
        shift = jnp.where(gate == 2, 0.0, 0.5)
        pieces = []
        for p in range(width // LANES):
            lanes = slice(p * LANES, (p + 1) * LANES)
            z = bias_ref[bias_row:bias_row + 1, pl.ds(pl.multiple_of(row * width, LANES) + p * LANES, LANES)]
            for a in addends:
                z = z + a[p * LANES // part_n, :, pl.ds(p * LANES % part_n, LANES)]
            act = jnp.tanh(z * scale) * scale + shift
            f = pltpu.roll(act, LANES - 1, 1)
            g = pltpu.roll(act, LANES - 2, 1)
            o = pltpu.roll(act, LANES - 3, 1)
            c_new = f * c_ref[cell, :, lanes] + act * g
            c_ref[cell, :, lanes] = c_new
            pieces.append((o * jnp.tanh(c_new)).astype(BF16))
        return dot(jnp.concatenate(pieces, axis=1), sel[...]).astype(BF16)

    def gates_one(k, slot):
        for s in range(SPLIT):
            mate_copy(k, slot, 1, s).wait_recv()
            across_copy(k, slot, s).wait_recv()
        h = gates(k, b1_ref, k, (zp.at[k, 3], p1r.at[k, slot, 1], yr.at[k, slot]))
        for s in range(SPLIT):
            for part in range(2):
                mate_copy(k, slot, part, s).wait_send()
            across_copy(k, slot, s).wait_send()
        return h

    def layer_one(n, carry):
        slot = n % 2
        for k in range(2):
            if k == 1:
                pl.when(n == 0)(lambda: load_wait('x1'))
                input_product(1, steps - 1 - n)
                pl.when(core != 0)(lambda: middle(0, slot))
                pl.when(n == 0)(lambda: load_wait('h1'))
                pl.when(n == steps - 1)(lambda: load_start('m1'))

            @pl.when(n > 0)
            def _(k=k):
                h_wait_recv(k, hist.at[k, n], slot)
            head(k, slot, hist.at[k, n], wh.at[k])
        for k in range(2):
            h = gates_one(k, slot)

            @pl.when(n > 0)
            def _(k=k):
                h_wait_send(k, hist.at[k, n], slot)
            hsend[k] = h
            h_start(k, hist.at[k, n + 1], (n + 1) % 2)

            @pl.when(n > 0)
            def _(k=k):
                forward(2 * n - 2 + k)

            if k == 0:
                move_copy(2 * n).start()
                move_copy(2 * n + 1).start()

            if k == 0:
                @pl.when(n < steps - 1)
                def _():
                    input_product(0, n + 1)
                pl.when(n == steps - 1)(lambda: load_start('m0'))
        return carry

    lax.fori_loop(0, steps, layer_one, 0)

    def mid_mate_copy(slot, part):
        return pltpu.make_async_remote_copy(
            src_ref=zp.at[1, 2 * part], dst_ref=m1r.at[slot, part],
            send_sem=m1_send.at[part], recv_sem=m1_recv.at[slot, part],
            device_id={'row': mate}, device_id_type=MESH)

    def mid_across_copy(slot):
        return pltpu.make_async_remote_copy(
            src_ref=zp.at[1, 1], dst_ref=myr.at[slot],
            send_sem=my_send, recv_sem=my_recv.at[slot],
            device_id={'row': across}, device_id_type=MESH)

    def mid_wait_send():
        for part in range(2):
            mid_mate_copy(0, part).wait_send()
        mid_across_copy(0).wait_send()

    def mid_product(t):
        slot = t % 3
        a = joined(hist.at[0, t + 1])
        b = joined(hist.at[1, steps - t])
        for idx in range(4):
            for s in range(SPLIT):
                z = dot(a, wx[0, idx, :, lanes_of(s)]) + dot(b, wx[1, idx, :, lanes_of(s)])
                if idx < 3:
                    zp[1, idx, s] = z
                else:
                    zm[t % 2, s] = z
            if idx % 2 == 0:
                mid_mate_copy(slot, idx // 2).start()
        mid_mate_copy(slot, 0).wait_recv()
        zp[1, 1] = zp[1, 1] + m1r[slot, 0]
        mid_across_copy(slot).start()

    def h2_copy(slot, i, p):
        return pltpu.make_async_remote_copy(
            src_ref=hsend.at[2], dst_ref=h2b.at[slot, p, row],
            send_sem=h2_send.at[i, p], recv_sem=h2_recv.at[slot, p, row],
            device_id={'col': far(i), 'row': (col + 2 * p) % n_row}, device_id_type=MESH)

    h2_stays = [row == (col + 2 * p) % n_row for p in range(2)]

    cross = 1 - (col // 2 - row // 2) * (col // 2 - row // 2)

    def h2_start(slot):
        for i in range(n_col):
            for q in range(2):
                p = (q + cross) % 2
                stays = (row == (col + 2 * p) % n_row) & (far(i) == col)
                pl.when(jnp.logical_not(stays))(lambda i=i, p=p: h2_copy(slot, i, p).start())
        for p in range(2):
            @pl.when(h2_stays[p])
            def _(p=p):
                h2b[slot, p, row] = hsend[2]

    def h2_wait_send(slot):
        for i in range(n_col):
            for p in range(2):
                pl.when(jnp.logical_not(h2_stays[p] & (far(i) == col)))(
                    lambda i=i, p=p: h2_copy(slot, i, p).wait_send())

    def h2_wait_recv(slot, p):
        stays = (row + 2 * p) % n_row == col
        for j in range(n_row):
            def wait(j=j):
                pltpu.make_async_remote_copy(
                    src_ref=hsend.at[2], dst_ref=h2b.at[slot, p, j],
                    send_sem=h2_send.at[0, 0], recv_sem=h2_recv.at[slot, p, j],
                    device_id={'col': col, 'row': row}, device_id_type=MESH).wait_recv()
            pl.when(jnp.logical_not(stays & (row == j)))(wait)

    def distance(r):
        return (r - col) * (r - col)

    nearer = jnp.where(distance(row) < distance((row + 2) % n_row), 0, 1)

    for k in range(2):
        forward(2 * steps - 2 + k)
    for k in range(2):
        h_wait_send(k, hist.at[k, steps], steps % 2)
    for name in ('m0', 'm1'):
        load_wait(name)
    mid_product(1)
    for k in range(2):
        h_wait_recv(k, hist.at[k, steps], steps % 2)
    mid_wait_send()
    mid_product(0)
    h2_load.wait()
    h0_copy.wait()
    moved_rows = wh2.at[1, pl.ds(pl.multiple_of(data * half, 16), half)]
    came_rows = wh2.at[1, pl.ds(pl.multiple_of((1 - data) * half, 16), half)]
    pltpu.make_async_remote_copy(
        src_ref=moved_rows, dst_ref=moved_rows, send_sem=move_send, recv_sem=move_recv.at[0],
        device_id={'row': across}, device_id_type=MESH).wait_send()
    pltpu.make_async_remote_copy(
        src_ref=moved_rows, dst_ref=came_rows, send_sem=relay_send, recv_sem=relay_recv,
        device_id={'data': 1 - data}, device_id_type=MESH).wait()

    def layer_two(n, carry):
        slot = n % 2

        parts = ((0, 1 - core), (3, core))

        def cols_of(part, s):
            return pl.ds(pl.multiple_of(part * width + s * part_n, LANES), part_n)

        pl.when(n > 0)(lambda: h2_wait_recv(slot, nearer))
        a = joined(h2b.at[slot, nearer])
        for idx, part in parts:
            for s in range(SPLIT):
                zp[0, idx, s] = dot(a, wh2[nearer, :, cols_of(part, s)])
        pl.when(n > 0)(lambda: h2_wait_recv(slot, 1 - nearer))
        a = joined(h2b.at[slot, 1 - nearer])
        todo = []

        def finish(idx, s, z):
            zp[0, idx, s] = zp[0, idx, s] + z
            if idx == 0:
                mate_copy(0, slot, 0, s).start()

        for idx, part in parts:
            for s in range(SPLIT):
                todo.append((idx, s, dot(a, wh2[1 - nearer, :, cols_of(part, s)])))
                if len(todo) > 1:
                    finish(*todo.pop(0))
        finish(*todo.pop(0))
        for s in range(SPLIT):
            mate_copy(0, slot, 0, s).wait_recv()
        mid_slot = n % 3
        mid_mate_copy(mid_slot, 1).wait_recv()
        mid_across_copy(mid_slot).wait_recv()
        h = gates(2, b2_ref, 0, (zp.at[0, 3], p1r.at[0, slot, 0], zm.at[slot],
                                 m1r.at[mid_slot, 1], myr.at[mid_slot]))
        for s in range(SPLIT):
            mate_copy(0, slot, 0, s).wait_send()

        @pl.when(n > 0)
        def _():
            h2_wait_send(slot)
        hsend[2] = h
        out_ref[n] = h

        @pl.when(n < steps - 1)
        def _():
            h2_start(1 - slot)

        @pl.when(n < steps - 2)
        def _():
            mid_wait_send()
            mid_product(n + 2)
        return carry

    lax.fori_loop(0, steps, layer_two, 0)
    mid_wait_send()
    for k in range(3):
        c_out[k] = moved(c_ref[k], sel[...])


def solution(mesh):
    n_data = mesh.shape['data']
    n_row = mesh.shape['row']
    n_col = mesh.shape['col']
    spec_seq = P(None, 'data', 'row')
    spec_weight = P(None, 'row', 'col')
    spec_out = P(None, 'data', ('col', 'row'))

    def local(x_rows, w_x1, w_h1, b_1, w_x2, w_h2, b_2, h_zero, c_zero):
        steps, batch, d_row = x_rows.shape
        unit_n = d_row // n_col
        width = 4 * unit_n
        vmem = pl.BlockSpec(memory_space=pltpu.VMEM)
        hbm = pl.BlockSpec(memory_space=pl.ANY)
        dma = pltpu.SemaphoreType.DMA
        out = pl.pallas_call(
            functools.partial(lstm_kernel, steps, n_data, n_row, n_col),
            out_shape=(jax.ShapeDtypeStruct((steps, batch, unit_n), BF16),
                       jax.ShapeDtypeStruct((3, batch, unit_n), F32)),
            in_specs=[vmem, hbm, hbm, hbm, hbm, vmem, vmem, vmem, vmem],
            out_specs=(vmem, vmem),
            scratch_shapes=[
                pltpu.VMEM((2, 4, d_row, width), BF16),
                pltpu.VMEM((2, 4, d_row, width), BF16),
                pltpu.VMEM((2, d_row, 2 * width), BF16),
                pltpu.VMEM((2, steps + 1, n_row, batch, unit_n), BF16),
                pltpu.VMEM((2, 2, n_row, batch, unit_n), BF16),
                pltpu.VMEM((2, 4, SPLIT, batch, width // SPLIT), F32),
                pltpu.VMEM((2, 2, 2, SPLIT, batch, width // SPLIT), F32),
                pltpu.VMEM((2, 2, SPLIT, batch, width // SPLIT), F32),
                pltpu.VMEM((2, SPLIT, batch, width // SPLIT), F32),
                pltpu.VMEM((3, 2, SPLIT, batch, width // SPLIT), F32),
                pltpu.VMEM((3, SPLIT, batch, width // SPLIT), F32),
                pltpu.VMEM((3, batch, unit_n), BF16),
                pltpu.VMEM((width, unit_n), BF16),
                pltpu.VMEM((unit_n, width), BF16),
                pltpu.VMEM((3, batch, unit_n), F32),
                pltpu.VMEM((3, batch, width), F32),
                dma((2,)),
                dma((7, 4)), dma((2, 2, SPLIT)), dma((2, 2, 2, SPLIT)), dma((2, SPLIT)), dma((2, 2, SPLIT)),
                dma((2,)), dma((3, 2)), dma, dma((3,)),
                dma((2, n_col)), dma((2, 2, n_row)), dma((n_col, 2)), dma((2, 2, n_row)),
                dma((2,)), dma, dma((8,)), dma, dma,
            ],
            compiler_params=pltpu.CompilerParams(
                collective_id=0, has_side_effects=True, vmem_limit_bytes=60 * 1024 * 1024),
        )(x_rows, w_x1, w_h1, w_x2, w_h2, b_1, b_2[None], h_zero, c_zero)

        def copy_out(a_ref, b_ref, a_out, b_out):
            a_out[...] = a_ref[...]
            b_out[...] = b_ref[...]

        return pl.pallas_call(
            copy_out, in_specs=[vmem, vmem], out_specs=(vmem, vmem),
            out_shape=(jax.ShapeDtypeStruct((steps, batch, unit_n), BF16),
                       jax.ShapeDtypeStruct((3, batch, unit_n), F32)))(*out)

    return jax.shard_map(local, mesh=mesh,
                         in_specs=(spec_seq, spec_weight, spec_weight, P(None, 'col'), spec_weight,
                                   P('row', 'col'), P('col'), spec_seq, spec_seq),
                         out_specs=(spec_out, spec_out), check_vma=False)
```
